128 devices in a mesh: tm: 64 (over y, z, x_lo, core), asset: 2 (over x_hi).
Axes of the slice: x: 4 (x_hi: 2, x_lo: 2; x = x_hi * 2 + x_lo), y: 4, z: 4, core: 2. Of those that a mesh axis runs over, the one named last changes fastest.
Arguments:
- tick_bars: float32 [2, 64, 61440], P('asset', 'tm'), may hold values from -20 to 20
- prior_bars: float32 [2, 64, 1600], P('asset', 'tm'), may hold values from -20 to 20, as said below
Outputs:
- connectedness: float32 [192, 8192], P('tm', 'asset')
The draws below stay inside these ranges and needn't reach their ends.
Inputs may be any that keep to these rules, and one draw needn't show every extreme that they name: `prior_bars`: bar returns of the same assets.
All inputs are finite; a program needn't handle non-finite values.
Results may differ from the reference program's by a relative error of at most 0.0014.
Values may be sent and summed in bfloat16 or wider, within the bound.
A program may use at most 64 MiB of HBM per device.

```python
import math
import jax
import jax.numpy as jnp
from jax import lax

ASSETS = 8192
SPAN = 30
STRIDE = 5
LEAD = 25
BARS = 960
WINDOWS = 192
N_TM = 64


cluster_count = 16


def return_draw(key, count, salt):
    tile_cols = ASSETS // 2
    log_scale = jax.random.uniform(jax.random.fold_in(key, 11), (2, 1, tile_cols), jnp.float32, math.log(0.1), math.log(3.0))
    scales = jnp.exp(log_scale)
    first_pick = jax.random.randint(jax.random.fold_in(key, 13), (2, tile_cols), 0, cluster_count)
    second_pick = jax.random.randint(jax.random.fold_in(key, 14), (2, tile_cols), 0, cluster_count)
    cluster = jnp.minimum(first_pick, second_pick)
    signs = 2.0 * jax.random.randint(jax.random.fold_in(key, 15), (2, 1, tile_cols), 0, 2).astype(jnp.float32) - 1.0
    loading = signs * jax.random.uniform(jax.random.fold_in(key, 16), (2, 1, tile_cols), jnp.float32, 0.3, 1.3)
    noise_key = jax.random.fold_in(key, salt)
    sector_moves = jnp.clip(jax.random.normal(jax.random.fold_in(noise_key, 3), (count, cluster_count), jnp.float32), -3.0, 3.0)
    sector_vol = jnp.exp(jax.random.uniform(jax.random.fold_in(noise_key, 4), (count, cluster_count), jnp.float32, math.log(0.4), math.log(2.0)))
    sector_factor = sector_moves * sector_vol
    asset_factor = jnp.transpose(sector_factor[:, cluster], (1, 0, 2))
    idiosyncratic = jnp.clip(jax.random.normal(noise_key, (2, count, tile_cols), jnp.float32), -4.0, 4.0)
    drawn = scales * (loading * asset_factor + idiosyncratic)
    drawn = jnp.clip(drawn, -19.5, 19.5)
    group_cols = ASSETS // (2 * N_TM)
    grid = drawn.reshape(2, count, N_TM, group_cols)
    return jnp.transpose(grid, (0, 2, 1, 3)).reshape(2, N_TM, count * group_cols).astype(jnp.float32)


def draw_tick_bars(key, part):
    return return_draw(key, BARS, 21)


def draw_prior_bars(key, part):
    return return_draw(key, LEAD, 22)


def setup_inputs(seed: int = 0) -> dict:
    streams_of = jax.random.split(jax.random.key(seed), 3)
    return {
        "tick_bars": draw_tick_bars(jax.random.fold_in(streams_of[2], 71), 0),
        "prior_bars": draw_prior_bars(jax.random.fold_in(streams_of[2], 71), 0),
    }


FLOOR_SQUARES = 1.0

def standardize(values):
    centred = values - lax.optimization_barrier(jnp.mean(values, axis=0, keepdims=True))
    squares = lax.optimization_barrier(jnp.sum(centred * centred, axis=0, keepdims=True))
    return (centred * lax.rsqrt(jnp.maximum(squares, FLOOR_SQUARES))).astype(jnp.bfloat16)

def unfold(packed, count):
    group_cols = ASSETS // (2 * N_TM)
    grid = packed.reshape(2, N_TM, count, group_cols)
    return jnp.transpose(grid, (2, 0, 1, 3)).reshape(count, ASSETS)

def reference(tick_bars, prior_bars):
    series_now = unfold(tick_bars, BARS)
    series_prior = unfold(prior_bars, LEAD)
    series = jnp.concatenate([series_prior, series_now], axis=0)
    block_rows = min(2048, ASSETS)

    def one_window(window_index):
        values = lax.dynamic_slice_in_dim(series, window_index * STRIDE, SPAN, 0)
        scaled = standardize(values).astype(jnp.float32)
        pieces = []
        for offset in range(0, ASSETS, block_rows):
            correlation = jnp.dot(scaled[:, offset:offset + block_rows].T, scaled, preferred_element_type=jnp.float32)
            magnitude = jnp.abs(correlation.astype(jnp.bfloat16)).astype(jnp.float32)
            pieces.append(lax.optimization_barrier(jnp.sum(magnitude, axis=1)))
        return jnp.concatenate(pieces) * (math.sqrt(SPAN) / ASSETS)
    return lax.map(one_window, jnp.arange(WINDOWS, dtype=jnp.int32))
```

```python
import functools
import math

import jax
import jax.numpy as jnp
from jax import lax
from jax.experimental import pallas as pl
from jax.experimental.pallas import tpu as pltpu
from jax.sharding import PartitionSpec as P

ASSETS = 8192
SPAN = 30
STRIDE = 5
WIN_DEV = 3
LEAD = 25
FLOOR_SQUARES = 1.0

MESH = pl.DeviceIdType.MESH
TILE = ASSETS // 2
GROUPS = 64
GROUP_COLS = TILE // GROUPS
BLOCK_BARS = WIN_DEV * STRIDE
LEAD_ROWS = 13
TICK_ROWS = 480
PAD_ROWS = 16
SERIES_ROWS = LEAD_ROWS + TICK_ROWS + PAD_ROWS - LEAD_ROWS
MSG_ROWS = 21
SLOT_ROWS = 24
BLOCK = 256
HALF = TILE // 2
EXT = TILE + HALF
UNROLL = 2


def place():
    tm = lax.axis_index("tm")
    return tm // 2, lax.rem(tm, 2), lax.axis_index("asset")


def gather_kernel(tick_ref, prior_ref, own_ref, other_ref, series, load_sem, send_sem, pass_sem, own_sem, other_sem):
    pair, core, half = place()
    me = pair * 2 + core
    loads = [
        pltpu.make_async_copy(prior_ref.at[pl.ds(0, LEAD_ROWS)], series.at[pl.ds(0, LEAD_ROWS)], load_sem.at[0]),
        pltpu.make_async_copy(tick_ref, series.at[pl.ds(LEAD_ROWS, TICK_ROWS)], load_sem.at[1]),
        pltpu.make_async_copy(
            prior_ref.at[pl.ds(LEAD_ROWS, PAD_ROWS - LEAD_ROWS)],
            series.at[pl.ds(LEAD_ROWS + TICK_ROWS, PAD_ROWS - LEAD_ROWS)],
            load_sem.at[2],
        ),
    ]
    for load in loads:
        load.start()

    barrier = pltpu.get_barrier_semaphore()

    def greet(g, carry):
        @pl.when(jnp.logical_or(g != me, core != half))
        def _():
            pl.semaphore_signal(barrier, inc=1, device_id=(g, core), device_id_type=MESH)

        return carry

    lax.fori_loop(0, GROUPS, greet, 0)
    pl.semaphore_signal(barrier, inc=1, device_id=(pair * 2 + 1 - core, half), device_id_type=MESH)
    pl.semaphore_wait(barrier, GROUPS + jnp.where(core == half, 0, 1))
    for load in loads:
        load.wait()

    def message(k):
        target_pair = lax.bitwise_xor(pair, k // 2)
        target_half = lax.bitwise_xor(half, lax.rem(k, 2))
        start = (BLOCK_BARS * (2 * target_pair + target_half) + 1) // 2
        return target_pair, target_half, series.at[pl.ds(start, MSG_ROWS)]

    def remote(k):
        target_pair, target_half, src = message(k)
        return pltpu.make_async_remote_copy(
            src_ref=src,
            dst_ref=own_ref.at[me, pl.ds(0, MSG_ROWS)],
            send_sem=send_sem.at[k],
            recv_sem=own_sem.at[me],
            device_id=(target_pair * 2 + half, target_half),
            device_id_type=MESH,
        )

    def local():
        _, _, src = message(0)
        return pltpu.make_async_copy(src, own_ref.at[me, pl.ds(0, MSG_ROWS)], own_sem.at[me])

    @pl.when(core == half)
    def _():
        local().start()

    @pl.when(core != half)
    def _():
        remote(0).start()

    def send(k, carry):
        remote(k).start()
        return carry

    lax.fori_loop(1, GROUPS, send, 0)

    def passing(g):
        return pltpu.make_async_remote_copy(
            src_ref=own_ref.at[g, pl.ds(0, MSG_ROWS)],
            dst_ref=other_ref.at[g, pl.ds(0, MSG_ROWS)],
            send_sem=pass_sem.at[g],
            recv_sem=other_sem.at[g],
            device_id=(pair * 2 + 1 - core, half),
            device_id_type=MESH,
        )

    def slot(j):
        return lax.bitwise_xor(me, j)

    def forward(j, carry):
        g = slot(j)
        ref = own_ref.at[g, pl.ds(0, MSG_ROWS)]
        pltpu.make_async_copy(ref, ref, own_sem.at[g]).wait()
        passing(g).start()
        return carry

    lax.fori_loop(0, GROUPS, forward, 0)

    @pl.when(core != half)
    def _():
        remote(0).wait_send()

    def finish_send(k, carry):
        remote(k).wait_send()
        return carry

    lax.fori_loop(1, GROUPS, finish_send, 0)

    def finish_pass(j, carry):
        passing(slot(j)).wait()
        return carry

    lax.fori_loop(0, GROUPS, finish_pass, 0)


def gather(tick_bars, prior_bars):
    tick = tick_bars.reshape(TICK_ROWS, 1, 128)
    prior = jnp.pad(prior_bars.reshape(-1), (GROUP_COLS, PAD_ROWS * 128 - GROUP_COLS - LEAD * GROUP_COLS))
    prior = prior.reshape(PAD_ROWS, 1, 128)
    slots = jax.ShapeDtypeStruct((GROUPS, SLOT_ROWS, 1, 128), jnp.float32)
    own, other = pl.pallas_call(
        gather_kernel,
        out_shape=(slots, slots),
        in_specs=[pl.BlockSpec(memory_space=pl.ANY)] * 2,
        out_specs=[pl.BlockSpec(memory_space=pl.ANY)] * 2,
        scratch_shapes=[
            pltpu.VMEM((SERIES_ROWS, 1, 128), jnp.float32),
            pltpu.SemaphoreType.DMA((3,)),
            pltpu.SemaphoreType.DMA((GROUPS,)),
            pltpu.SemaphoreType.DMA((GROUPS,)),
            pltpu.SemaphoreType.DMA((GROUPS,)),
            pltpu.SemaphoreType.DMA((GROUPS,)),
        ],
        compiler_params=pltpu.CompilerParams(collective_id=0, has_side_effects=True),
        name="gather_bars",
    )(tick, prior)
    return own.reshape(GROUPS, SLOT_ROWS, 128), other.reshape(GROUPS, SLOT_ROWS, 128)


def magnitudes(lhs, rhs):
    return jnp.abs(
        lax.dot_general(lhs, rhs, (((1,), (0,)), ((), ())), preferred_element_type=jnp.float32)
    )


def fold_rows(a):
    return jnp.sum(a.reshape(a.shape[0] // 8, 8, a.shape[1]), axis=0)


def unpack_bars(raw_ref, bars, half):
    low = lax.broadcasted_iota(jnp.int32, (SLOT_ROWS, 128), 1) < GROUP_COLS

    def aligned(p, carry):
        a, b = raw_ref[2 * p], raw_ref[2 * p + 1]
        cols = pl.ds(pl.multiple_of(p * 128, 128), 128)
        bars[0, :, cols] = jnp.where(low, a, pltpu.roll(b, GROUP_COLS, 1))
        bars[1, :, cols] = jnp.where(low, pltpu.roll(a, GROUP_COLS, 1), b)
        return carry

    def shifted(p, carry):
        a, b = raw_ref[2 * p], raw_ref[2 * p + 1]
        cols = pl.ds(pl.multiple_of(p * 128, 128), 128)
        bars[0, :, cols] = jnp.where(low, pltpu.roll(a, GROUP_COLS, 1), b)
        even = jnp.where(low, a, pltpu.roll(b, GROUP_COLS, 1))
        bars[1, :, cols] = pltpu.roll(even, SLOT_ROWS - 1, 0)
        return carry

    @pl.when(half == 1)
    def _():
        lax.fori_loop(0, GROUPS // 2, aligned, 0, unroll=4)

    @pl.when(half == 0)
    def _():
        lax.fori_loop(0, GROUPS // 2, shifted, 0, unroll=4)


def standardize(bars, scaled, width=512):
    valid = lax.broadcasted_iota(jnp.int32, (16, width), 0) < SPAN // 2

    def chunk(j, carry):
        cols = pl.ds(pl.multiple_of(j * width, width), width)
        for w in range(WIN_DEV):
            first = w * STRIDE
            even = jnp.where(valid, bars[0, pl.ds((first + 1) // 2, 16), cols], 0.0)
            odd = jnp.where(valid, bars[1, pl.ds(first // 2, 16), cols], 0.0)
            mean = (jnp.sum(even, axis=0, keepdims=True) + jnp.sum(odd, axis=0, keepdims=True)) * (1.0 / SPAN)
            even = jnp.where(valid, even - mean, 0.0)
            odd = jnp.where(valid, odd - mean, 0.0)
            squares = jnp.sum(even * even, axis=0, keepdims=True) + jnp.sum(odd * odd, axis=0, keepdims=True)
            scale = lax.rsqrt(jnp.maximum(squares, FLOOR_SQUARES))
            scaled[pl.ds(32 * w, 16), cols] = (even * scale).astype(jnp.bfloat16)
            scaled[pl.ds(32 * w + 16, 16), cols] = (odd * scale).astype(jnp.bfloat16)
        return carry

    lax.fori_loop(0, TILE // width, chunk, 0)
    scaled[pl.ds(96, 32), :] = jnp.zeros((32, scaled.shape[1]), jnp.bfloat16)


def connect_kernel(own_raw, other_raw, out_ref, bars, own, other, lhs_ref, rows, row_line, own_cols, other_cols):
    _, core, half = place()
    unpack_bars(own_raw, bars, half)
    standardize(bars, own)
    unpack_bars(other_raw, bars, half)
    standardize(bars, other)
    own[:, TILE:EXT] = own[:, 0:HALF]
    lane = lax.broadcasted_iota(jnp.int32, (128, 128), 1)

    def transpose_block(p, carry):
        at = pl.ds(pl.multiple_of(p * 128, 128), 128)
        turned = own[:, at].T
        for w in range(WIN_DEV):
            keep = (lane // 32 == w).astype(jnp.float32).astype(jnp.bfloat16)
            lhs_ref[w, at, :] = turned * keep
        return carry

    lax.fori_loop(0, TILE // 128, transpose_block, 0, unroll=2)
    own_cols[...] = jnp.zeros_like(own_cols)
    other_cols[...] = jnp.zeros_like(other_cols)

    def within(i, carry):
        row0 = pl.multiple_of(i * BLOCK, BLOCK)
        for w in range(WIN_DEV):
            lhs = lhs_ref[w, pl.ds(row0, BLOCK), :]
            total = None
            for d in range(0, HALF, BLOCK):
                cols = pl.ds(pl.multiple_of(row0 + d, BLOCK), BLOCK)
                a = magnitudes(lhs, own[:, cols])
                part = a[:, :128] + a[:, 128:]
                total = part if total is None else total + part
                if d:
                    own_cols[w, :, cols] += fold_rows(a)
            rows[w, pl.ds(row0, BLOCK), :] = total
            low = lax.rem(i, 8)
            across = pl.ds(pl.multiple_of(low * BLOCK + (i // 8) * 128, 128), 128)
            cols = pl.ds(pl.multiple_of((low + 8) * BLOCK, BLOCK), BLOCK)
            a = magnitudes(lhs_ref[w, across, :], own[:, cols])
            rows[w, across, :] += a[:, :128] + a[:, 128:]
            own_cols[w, :, cols] += fold_rows(a)
        return carry

    lax.fori_loop(0, TILE // BLOCK, within, 0, unroll=UNROLL)

    def between(i, carry):
        row0 = pl.multiple_of(i * BLOCK, BLOCK)
        col0 = lax.rem(i // 8 + core, 2) * HALF
        for w in range(WIN_DEV):
            lhs = lhs_ref[w, pl.ds(row0, BLOCK), :]
            total = rows[w, pl.ds(row0, BLOCK), :]
            for d in range(0, HALF, BLOCK):
                cols = pl.ds(pl.multiple_of(col0 + d, BLOCK), BLOCK)
                a = magnitudes(lhs, other[:, cols])
                total = total + (a[:, :128] + a[:, 128:])
                other_cols[w, :, cols] += fold_rows(a)
            for q in range(0, BLOCK, 128):
                line = jnp.sum(total[q : q + 128].T, axis=0, keepdims=True)
                row_line[pl.ds(w, 1), pl.ds(pl.multiple_of(row0 + q, 128), 128)] = line
        return carry

    lax.fori_loop(0, TILE // BLOCK, between, 0, unroll=UNROLL)
    scale = math.sqrt(SPAN) / ASSETS
    for w in range(WIN_DEV):
        one = pl.ds(w, 1)
        out_ref[1, one, :] = jnp.sum(other_cols[w], axis=0, keepdims=True) * scale
        mine = row_line[one, :] + jnp.sum(own_cols[w, :, 0:TILE], axis=0, keepdims=True)
        out_ref[0, one, HALF:TILE] = mine[:, HALF:] * scale
        wrapped = jnp.sum(own_cols[w, :, TILE:EXT], axis=0, keepdims=True)
        out_ref[0, one, 0:HALF] = (mine[:, :HALF] + wrapped) * scale


def connect(own_raw, other_raw):
    return pl.pallas_call(
        connect_kernel,
        out_shape=jax.ShapeDtypeStruct((2, WIN_DEV, TILE), jnp.float32),
        in_specs=[pl.BlockSpec(memory_space=pltpu.VMEM)] * 2,
        out_specs=pl.BlockSpec(memory_space=pltpu.VMEM),
        scratch_shapes=[
            pltpu.VMEM((2, SLOT_ROWS, TILE), jnp.float32),
            pltpu.VMEM((128, EXT), jnp.bfloat16),
            pltpu.VMEM((128, TILE), jnp.bfloat16),
            pltpu.VMEM((WIN_DEV, TILE, 128), jnp.bfloat16),
            pltpu.VMEM((WIN_DEV, TILE, 128), jnp.float32),
            pltpu.VMEM((8, TILE), jnp.float32),
            pltpu.VMEM((WIN_DEV, 8, EXT), jnp.float32),
            pltpu.VMEM((WIN_DEV, 8, TILE), jnp.float32),
        ],
        compiler_params=pltpu.CompilerParams(vmem_limit_bytes=48 * 2**20),
        name="connect",
    )(own_raw, other_raw)


def shards(tick_bars, prior_bars):
    own_raw, other_raw = gather(tick_bars, prior_bars)
    sums = connect(own_raw, other_raw)
    main = [(4 * pair + 2 * core + half, 4 * pair + 2 * half + core) for pair in range(32) for core in range(2) for half in range(2)]
    side = [(4 * pair + 2 * core + half, 4 * pair + 2 * half + 1 - core) for pair in range(32) for core in range(2) for half in range(2)]
    first = lax.ppermute(sums[0], ("tm", "asset"), main)
    second = lax.ppermute(sums[1], ("tm", "asset"), side)
    return first + second


def solution(mesh):
    in_specs = (P("asset", "tm", None), P("asset", "tm", None))
    out_specs = P("tm", "asset")
    return jax.shard_map(shards, mesh=mesh, in_specs=in_specs, out_specs=out_specs, check_vma=False)
```

```python
import functools
import math

import jax
import jax.numpy as jnp
from jax import lax
from jax.experimental import pallas as pl
from jax.experimental.pallas import tpu as pltpu
from jax.sharding import PartitionSpec as P

ASSETS = 8192
SPAN = 30
STRIDE = 5
WIN_DEV = 3
LEAD = 25
FLOOR_SQUARES = 1.0

MESH = pl.DeviceIdType.MESH
TILE = ASSETS // 2
GROUPS = 64
GROUP_COLS = TILE // GROUPS
BLOCK_BARS = WIN_DEV * STRIDE
LEAD_ROWS = 13
TICK_ROWS = 480
SERIES_ROWS = LEAD_ROWS + TICK_ROWS + 1
MSG_ROWS = 21
SLOT_ROWS = 24
BLOCK = 256
HALF = TILE // 2
EXT = TILE + HALF
UNROLL = 4


def place():
    tm = lax.axis_index("tm")
    return tm // 2, lax.rem(tm, 2), lax.axis_index("asset")


def magnitudes(lhs, rhs):
    return jnp.abs(
        lax.dot_general(lhs, rhs, (((1,), (0,)), ((), ())), preferred_element_type=jnp.float32)
    )


def fold_rows(a):
    return jnp.sum(a.reshape(a.shape[0] // 8, 8, a.shape[1]), axis=0)


def prepare(raw_ref, bars, scaled, chunk, half):
    low = lax.broadcasted_iota(jnp.int32, (SLOT_ROWS, 128), 1) < GROUP_COLS
    for p in range(4):
        slot = chunk * 8 + 2 * p
        a, b = raw_ref[slot, :, 0, :], raw_ref[slot + 1, :, 0, :]
        cols = pl.ds(p * 128, 128)
        even = jnp.where(low, a, pltpu.roll(b, GROUP_COLS, 1))
        odd = jnp.where(low, pltpu.roll(a, GROUP_COLS, 1), b)
        aligned = half == 1
        bars[0, :, cols] = jnp.where(aligned, even, odd)
        bars[1, :, cols] = jnp.where(aligned, odd, pltpu.roll(even, SLOT_ROWS - 1, 0))
    valid = lax.broadcasted_iota(jnp.int32, (16, 512), 0) < SPAN // 2
    at = pl.ds(pl.multiple_of(chunk * 512, 512), 512)
    for w in range(WIN_DEV):
        first = w * STRIDE
        even = jnp.where(valid, bars[0, pl.ds((first + 1) // 2, 16), :], 0.0)
        odd = jnp.where(valid, bars[1, pl.ds(first // 2, 16), :], 0.0)
        mean = (jnp.sum(even, axis=0, keepdims=True) + jnp.sum(odd, axis=0, keepdims=True)) * (1.0 / SPAN)
        even = jnp.where(valid, even - mean, 0.0)
        odd = jnp.where(valid, odd - mean, 0.0)
        squares = jnp.sum(even * even, axis=0, keepdims=True) + jnp.sum(odd * odd, axis=0, keepdims=True)
        scale = lax.rsqrt(jnp.maximum(squares, FLOOR_SQUARES))
        scaled[pl.ds(32 * w, 16), at] = (even * scale).astype(jnp.bfloat16)
        scaled[pl.ds(32 * w + 16, 16), at] = (odd * scale).astype(jnp.bfloat16)


def turn(scaled, lhs_ref, chunk):
    lane = lax.broadcasted_iota(jnp.int32, (128, 128), 1)
    for p in range(4):
        at = pl.ds(pl.multiple_of(chunk * 512 + p * 128, 128), 128)
        turned = scaled[:, at].T
        for w in range(WIN_DEV):
            keep = (lane // 32 == w).astype(jnp.float32).astype(jnp.bfloat16)
            lhs_ref[w, at, :] = turned * keep


def kernel(
    tick_ref, prior_ref, out_ref, series, own_raw, other_raw, bars, own, other, lhs_ref, rows, own_cols, other_cols, result, arrived,
    load_sem, send_sem, pass_sem, own_sem, other_sem, result_send, result_recv,
):
    pair, core, half = place()
    me = pair * 2 + core
    sibling = pair * 2 + 1 - core
    load = pltpu.make_async_copy(tick_ref, series.at[pl.ds(LEAD_ROWS, TICK_ROWS)], load_sem)
    load.start()

    barrier = pltpu.get_barrier_semaphore()

    def greet(g, carry):
        @pl.when(jnp.logical_or(g != me, core != half))
        def _():
            pl.semaphore_signal(barrier, inc=1, device_id=(g, core), device_id_type=MESH)

        return carry

    lax.fori_loop(0, GROUPS, greet, 0)
    pl.semaphore_signal(barrier, inc=1, device_id=(sibling, half), device_id_type=MESH)

    low = lax.broadcasted_iota(jnp.int32, (1, 128), 1) < GROUP_COLS
    before = jnp.zeros((1, 128), jnp.float32)
    for r in range(LEAD_ROWS):
        now = pltpu.roll(prior_ref[pl.ds(r, 1), :], GROUP_COLS, 1)
        series[r] = jnp.where(low, before, now)
        before = now
    series[LEAD_ROWS + TICK_ROWS] = jnp.zeros((1, 128), jnp.float32)
    own[pl.ds(96, 32), :] = jnp.zeros((32, TILE), jnp.bfloat16)
    other[pl.ds(96, 32), :] = jnp.zeros((32, TILE), jnp.bfloat16)
    own_cols[...] = jnp.zeros_like(own_cols)
    other_cols[...] = jnp.zeros_like(other_cols)

    pl.semaphore_wait(barrier, GROUPS + jnp.where(core == half, 0, 1))
    load.wait()

    def message(k):
        target_pair = lax.bitwise_xor(pair, k // 2)
        target_half = lax.bitwise_xor(half, lax.rem(k, 2))
        start = (BLOCK_BARS * (2 * target_pair + target_half) + 1) // 2
        return target_pair, target_half, series.at[pl.ds(start, MSG_ROWS)]

    def remote(k):
        target_pair, target_half, src = message(k)
        return pltpu.make_async_remote_copy(
            src_ref=src,
            dst_ref=own_raw.at[me, pl.ds(0, MSG_ROWS)],
            send_sem=send_sem.at[k],
            recv_sem=own_sem.at[me],
            device_id=(target_pair * 2 + half, target_half),
            device_id_type=MESH,
        )

    @pl.when(core == half)
    def _():
        _, _, src = message(0)
        pltpu.make_async_copy(src, own_raw.at[me, pl.ds(0, MSG_ROWS)], own_sem.at[me]).start()

    @pl.when(core != half)
    def _():
        remote(0).start()

    def send(k, carry):
        remote(k).start()
        return carry

    lax.fori_loop(1, GROUPS, send, 0)

    def passing(g):
        return pltpu.make_async_remote_copy(
            src_ref=own_raw.at[g, pl.ds(0, MSG_ROWS)],
            dst_ref=other_raw.at[g, pl.ds(0, MSG_ROWS)],
            send_sem=pass_sem.at[g],
            recv_sem=other_sem.at[g],
            device_id=(sibling, half),
            device_id_type=MESH,
        )

    def receive(q, carry):
        chunk = lax.bitwise_xor(me // 8, q)
        for j in range(8):
            g = chunk * 8 + j
            ref = own_raw.at[g, pl.ds(0, MSG_ROWS)]
            pltpu.make_async_copy(ref, ref, own_sem.at[g]).wait()
            passing(g).start()
        prepare(own_raw, bars, own, chunk, half)
        turn(own, lhs_ref, chunk)
        return carry

    first_half = me // 32

    def square(h):
        base = h * 8

        def step(i, carry):
            row0 = pl.multiple_of((base + i) * BLOCK, BLOCK)
            for w in range(WIN_DEV):
                lhs = lhs_ref[w, pl.ds(row0, BLOCK), :]
                total = None
                for d in range(4):
                    cols = pl.ds(pl.multiple_of((base + lax.rem(i + d, 8)) * BLOCK, BLOCK), BLOCK)
                    a = magnitudes(lhs, own[:, cols])
                    part = a[:, :128] + a[:, 128:]
                    total = part if total is None else total + part
                    if d:
                        own_cols[w, :, cols] += fold_rows(a)
                rows[w, pl.ds(row0, BLOCK), :] = total
                near = lax.rem(i, 4)
                across = pl.ds(pl.multiple_of((base + near) * BLOCK + (i // 4) * 128, 128), 128)
                cols = pl.ds(pl.multiple_of((base + near + 4) * BLOCK, BLOCK), BLOCK)
                a = magnitudes(lhs_ref[w, across, :], own[:, cols])
                rows[w, across, :] += a[:, :128] + a[:, 128:]
                own_cols[w, :, cols] += fold_rows(a)
            return carry

        lax.fori_loop(0, 8, step, 0, unroll=UNROLL)

    def stage(s, carry):
        lax.fori_loop(4 * s, 4 * s + 4, receive, 0)
        square(lax.bitwise_xor(first_half, s))
        return carry

    lax.fori_loop(0, 2, stage, 0)

    def across_halves(i, carry):
        row0 = pl.multiple_of(i * BLOCK, BLOCK)
        for w in range(WIN_DEV):
            lhs = lhs_ref[w, pl.ds(row0, BLOCK), :]
            total = rows[w, pl.ds(row0, BLOCK), :]
            for d in range(HALF, TILE, BLOCK):
                cols = pl.ds(d, BLOCK)
                a = magnitudes(lhs, own[:, cols])
                total = total + (a[:, :128] + a[:, 128:])
                own_cols[w, :, cols] += fold_rows(a)
            rows[w, pl.ds(row0, BLOCK), :] = total
        return carry

    lax.fori_loop(0, HALF // BLOCK, across_halves, 0, unroll=UNROLL)

    def receive_other(q, carry):
        chunk = lax.bitwise_xor(me // 8, q)
        for j in range(8):
            passing(chunk * 8 + j).wait()
        prepare(other_raw, bars, other, chunk, half)
        return carry

    lax.fori_loop(0, 8, receive_other, 0)

    def across_tiles(i, carry):
        row0 = pl.multiple_of(i * BLOCK, BLOCK)
        col0 = lax.rem(i // 8 + core, 2) * HALF
        for w in range(WIN_DEV):
            lhs = lhs_ref[w, pl.ds(row0, BLOCK), :]
            total = rows[w, pl.ds(row0, BLOCK), :]
            for d in range(0, HALF, BLOCK):
                cols = pl.ds(pl.multiple_of(col0 + d, BLOCK), BLOCK)
                a = magnitudes(lhs, other[:, cols])
                total = total + (a[:, :128] + a[:, 128:])
                other_cols[w, :, cols] += fold_rows(a)
            for q in range(0, BLOCK, 128):
                line = jnp.sum(total[q : q + 128].T, axis=0, keepdims=True)
                result[0, pl.ds(w, 1), pl.ds(pl.multiple_of(row0 + q, 128), 128)] = line
        return carry

    lax.fori_loop(0, TILE // BLOCK, across_tiles, 0, unroll=UNROLL)
    scale = math.sqrt(SPAN) / ASSETS
    for w in range(WIN_DEV):
        one = pl.ds(w, 1)
        result[1, one, :] = jnp.sum(other_cols[w], axis=0, keepdims=True) * scale
        result[0, one, :] = (result[0, one, :] + jnp.sum(own_cols[w], axis=0, keepdims=True)) * scale

    def result_copy(which):
        tile = core if which == 0 else 1 - core
        return pltpu.make_async_remote_copy(
            src_ref=result.at[which],
            dst_ref=arrived.at[which],
            send_sem=result_send.at[which],
            recv_sem=result_recv.at[which],
            device_id=(pair * 2 + half, tile),
            device_id_type=MESH,
        )

    result_copy(1).start()

    @pl.when(core != half)
    def _():
        result_copy(0).start()

    def finish_send(k, carry):
        remote(k).wait_send()
        return carry

    @pl.when(core != half)
    def _():
        remote(0).wait_send()

    lax.fori_loop(1, GROUPS, finish_send, 0)
    result_copy(1).wait()

    @pl.when(core != half)
    def _():
        result_copy(0).wait()
        out_ref[...] = arrived[0] + arrived[1]

    @pl.when(core == half)
    def _():
        out_ref[...] = result[0] + arrived[1]


def shards(tick_bars, prior_bars):
    slots = pltpu.VMEM((GROUPS, SLOT_ROWS, 1, 128), jnp.float32)
    prior = jnp.pad(prior_bars.reshape(1, -1), ((0, 0), (0, LEAD_ROWS * 128 - LEAD * GROUP_COLS))).reshape(LEAD_ROWS, 128)
    return pl.pallas_call(
        kernel,
        out_shape=jax.ShapeDtypeStruct((WIN_DEV, TILE), jnp.float32),
        in_specs=[pl.BlockSpec(memory_space=pl.ANY), pl.BlockSpec(memory_space=pltpu.VMEM)],
        out_specs=pl.BlockSpec(memory_space=pltpu.VMEM),
        scratch_shapes=[
            pltpu.VMEM((SERIES_ROWS, 1, 128), jnp.float32),
            slots,
            slots,
            pltpu.VMEM((2, SLOT_ROWS, 512), jnp.float32),
            pltpu.VMEM((128, TILE), jnp.bfloat16),
            pltpu.VMEM((128, TILE), jnp.bfloat16),
            pltpu.VMEM((WIN_DEV, TILE, 128), jnp.bfloat16),
            pltpu.VMEM((WIN_DEV, TILE, 128), jnp.float32),
            pltpu.VMEM((WIN_DEV, 8, TILE), jnp.float32),
            pltpu.VMEM((WIN_DEV, 8, TILE), jnp.float32),
            pltpu.VMEM((2, WIN_DEV, TILE), jnp.float32),
            pltpu.VMEM((2, WIN_DEV, TILE), jnp.float32),
            pltpu.SemaphoreType.DMA,
            pltpu.SemaphoreType.DMA((GROUPS,)),
            pltpu.SemaphoreType.DMA((GROUPS,)),
            pltpu.SemaphoreType.DMA((GROUPS,)),
            pltpu.SemaphoreType.DMA((GROUPS,)),
            pltpu.SemaphoreType.DMA((2,)),
            pltpu.SemaphoreType.DMA((2,)),
        ],
        compiler_params=pltpu.CompilerParams(collective_id=0, has_side_effects=True, vmem_limit_bytes=56 * 2**20),
        name="connect",
    )(tick_bars.reshape(TICK_ROWS, 1, 128), prior)


def solution(mesh):
    in_specs = (P("asset", "tm", None), P("asset", "tm", None))
    out_specs = P("tm", "asset")
    return jax.shard_map(shards, mesh=mesh, in_specs=in_specs, out_specs=out_specs, check_vma=False)
```

```python
import functools
import math

import jax
import jax.numpy as jnp
from jax import lax
from jax.experimental import pallas as pl
from jax.experimental.pallas import tpu as pltpu
from jax.sharding import PartitionSpec as P

ASSETS = 8192
SPAN = 30
STRIDE = 5
WIN_DEV = 3
LEAD = 25
FLOOR_SQUARES = 1.0

MESH = pl.DeviceIdType.MESH
TILE = ASSETS // 2
GROUPS = 64
GROUP_COLS = TILE // GROUPS
BLOCK_BARS = WIN_DEV * STRIDE
LEAD_ROWS = 13
TICK_ROWS = 480
SERIES_ROWS = LEAD_ROWS + TICK_ROWS + 1
MSG_ROWS = 21
SLOT_ROWS = 24
BLOCK = 256
HALF = TILE // 2
EXT = TILE + HALF
UNROLL = 4


def place():
    tm = lax.axis_index("tm")
    return tm // 2, lax.rem(tm, 2), lax.axis_index("asset")


def magnitudes(lhs, rhs):
    return jnp.abs(
        lax.dot_general(lhs, rhs, (((1,), (0,)), ((), ())), preferred_element_type=jnp.float32)
    )


def fold_rows(a):
    return jnp.sum(a.reshape(a.shape[0] // 8, 8, a.shape[1]), axis=0)


def prepare(raw_ref, bars, scaled, lhs_ref, chunk, half):
    low = lax.broadcasted_iota(jnp.int32, (SLOT_ROWS, 128), 1) < GROUP_COLS
    valid = lax.broadcasted_iota(jnp.int32, (16, 128), 0) < SPAN // 2
    aligned = half == 1
    for p in range(4):
        slot = chunk * 8 + 2 * p
        a, b = raw_ref[slot, :, 0, :], raw_ref[slot + 1, :, 0, :]
        even = jnp.where(low, a, pltpu.roll(b, GROUP_COLS, 1))
        odd = jnp.where(low, pltpu.roll(a, GROUP_COLS, 1), b)
        bars[0, p] = jnp.where(aligned, even, odd)
        bars[1, p] = jnp.where(aligned, odd, pltpu.roll(even, SLOT_ROWS - 1, 0))
    for p in range(4):
        at = pl.ds(pl.multiple_of(chunk * 512 + p * 128, 128), 128)
        parts = []
        for w in range(WIN_DEV):
            first = w * STRIDE
            even = jnp.where(valid, bars[0, p, pl.ds((first + 1) // 2, 16), :], 0.0)
            odd = jnp.where(valid, bars[1, p, pl.ds(first // 2, 16), :], 0.0)
            mean = jnp.sum(even + odd, axis=0, keepdims=True) * (1.0 / SPAN)
            even = jnp.where(valid, even - mean, 0.0)
            odd = jnp.where(valid, odd - mean, 0.0)
            squares = jnp.sum(even * even + odd * odd, axis=0, keepdims=True)
            scale = lax.rsqrt(jnp.maximum(squares, FLOOR_SQUARES))
            even, odd = (even * scale).astype(jnp.bfloat16), (odd * scale).astype(jnp.bfloat16)
            scaled[w, pl.ds(32 * w, 16), at] = even
            scaled[w, pl.ds(32 * w + 16, 16), at] = odd
            parts += [even, odd]
        parts.append(jnp.zeros((32, 128), jnp.bfloat16))
        lhs_ref[at, :] = jnp.concatenate(parts, axis=0).T


def kernel(
    tick_ref, prior_ref, out_ref, series, prior, own_raw, bars, own, other, lhs_ref, rows, own_cols, other_cols, result, arrived,
    load_sem, send_sem, own_sem, pass_sem, other_sem, result_send, result_recv,
):
    pair, core, half = place()
    me = pair * 2 + core
    sibling = pair * 2 + 1 - core
    prior_load = pltpu.make_async_copy(prior_ref, prior, load_sem.at[0])
    prior_load.start()
    load = pltpu.make_async_copy(tick_ref, series.at[pl.ds(LEAD_ROWS, TICK_ROWS)], load_sem.at[1])
    load.start()

    barrier = pltpu.get_barrier_semaphore()

    def greet(j, carry):
        g = lax.bitwise_xor(me, GROUPS - 1 - j)

        @pl.when(jnp.logical_or(g != me, core != half))
        def _():
            pl.semaphore_signal(barrier, inc=1, device_id=(g, core), device_id_type=MESH)

        return carry

    lax.fori_loop(0, GROUPS, greet, 0)
    pl.semaphore_signal(barrier, inc=1, device_id=(sibling, half), device_id_type=MESH)

    prior_load.wait()
    low = lax.broadcasted_iota(jnp.int32, (1, 128), 1) < GROUP_COLS
    series[0] = jnp.where(low, 0.0, pltpu.roll(prior[:, 0:128], GROUP_COLS, 1))
    for r in range(1, LEAD_ROWS):
        series[r] = prior[:, 128 * r - GROUP_COLS : 128 * r + GROUP_COLS]
    series[LEAD_ROWS + TICK_ROWS] = jnp.zeros((1, 128), jnp.float32)
    own_cols[...] = jnp.zeros_like(own_cols)
    other_cols[...] = jnp.zeros_like(other_cols)

    def clear(i, carry):
        at = pl.ds(pl.multiple_of(i * 256, 256), 256)
        for w in range(WIN_DEV):
            rows[w, at, :] = jnp.zeros((256, 128), jnp.float32)
            for first, last in ((0, 32 * w), (32 * w + 32, 128)):
                if last > first:
                    own[w, pl.ds(first, last - first), at] = jnp.zeros((last - first, 256), jnp.bfloat16)
                    other[w, pl.ds(first, last - first), at] = jnp.zeros((last - first, 256), jnp.bfloat16)
        return carry

    lax.fori_loop(0, TILE // 256, clear, 0)
    pl.semaphore_wait(barrier, GROUPS + jnp.where(core == half, 0, 1))
    load.wait()

    def message(k):
        target_pair = lax.bitwise_xor(pair, k // 2)
        target_half = lax.bitwise_xor(half, lax.rem(k, 2))
        start = (BLOCK_BARS * (2 * target_pair + target_half) + 1) // 2
        return target_pair, target_half, series.at[pl.ds(start, MSG_ROWS)]

    def remote(k):
        target_pair, target_half, src = message(k)
        return pltpu.make_async_remote_copy(
            src_ref=src,
            dst_ref=own_raw.at[me, pl.ds(0, MSG_ROWS)],
            send_sem=send_sem.at[k],
            recv_sem=own_sem.at[me],
            device_id=(target_pair * 2 + half, target_half),
            device_id_type=MESH,
        )

    @pl.when(core == half)
    def _():
        _, _, src = message(0)
        pltpu.make_async_copy(src, own_raw.at[me, pl.ds(0, MSG_ROWS)], own_sem.at[me]).start()

    @pl.when(core != half)
    def _():
        remote(0).start()

    def send(k, carry):
        remote(k).start()
        return carry

    lax.fori_loop(1, GROUPS, send, 0)

    def passing(q, w):
        at = pl.ds(pl.multiple_of(lax.bitwise_xor(me // 8, q) * 512, 512), 512)
        return pltpu.make_async_remote_copy(
            src_ref=own.at[w, pl.ds(32 * w, 32), at],
            dst_ref=other.at[w, pl.ds(32 * w, 32), at],
            send_sem=pass_sem.at[q, w],
            recv_sem=other_sem.at[q, w],
            device_id=(sibling, half),
            device_id_type=MESH,
        )

    def pass_on(q):
        for w in range(WIN_DEV):
            passing(q, w).start()

    def receive(q):
        chunk = lax.bitwise_xor(me // 8, q)
        for j in range(8):
            g = chunk * 8 + j
            ref = own_raw.at[g, pl.ds(0, MSG_ROWS)]
            pltpu.make_async_copy(ref, ref, own_sem.at[g]).wait()
        prepare(own_raw, bars, own, lhs_ref, chunk, half)
        return chunk

    def block(i):
        return pl.ds(pl.multiple_of(i * BLOCK, BLOCK), BLOCK)

    def pairs(w, row_at, col_at, right, cols):
        a = magnitudes(lhs_ref[row_at, :], right[w, :, col_at])
        if cols is not None:
            cols[w, :, col_at] += fold_rows(a)
        return a[:, :128] + a[:, 128:]

    def early(q, carry):
        chunk = receive(q)

        def with_earlier(r, carry):
            left = lax.bitwise_xor(me // 8, r)
            for w in range(WIN_DEV):
                for i in range(2):
                    row_at = block(2 * chunk + i)
                    rows[w, row_at, :] += pairs(w, row_at, block(2 * left), own, own_cols) + pairs(
                        w, row_at, block(2 * left + 1), own, own_cols
                    )
            return carry

        first, second = block(2 * chunk), block(2 * chunk + 1)
        for w in range(WIN_DEV):
            rows[w, first, :] += pairs(w, first, first, own, None) + pairs(w, first, second, own, own_cols)
            rows[w, second, :] += pairs(w, second, second, own, None)
        pass_on(q)
        lax.fori_loop(0, q, with_earlier, 0)
        return carry

    lax.fori_loop(0, 4, early, 0)
    first_half = me // 32
    near, far = first_half * 8, 8 - first_half * 8

    def late(q, carry):
        chunk = receive(q)
        for i in range(2):
            row_at = block(2 * chunk + i)
            for w in range(WIN_DEV):
                total = rows[w, row_at, :]
                for d in range(8):
                    total = total + pairs(w, row_at, block(near + d), own, own_cols)
                rows[w, row_at, :] = total
        pass_on(q)
        return carry

    lax.fori_loop(4, 8, late, 0)

    def receive_other(q, carry):
        for w in range(WIN_DEV):
            passing(q, w).wait_recv()
        return carry

    def sum_rows(w, i, total):
        for q in range(0, BLOCK, 128):
            at = pl.ds(pl.multiple_of(i * BLOCK + q, 128), 128)
            result[0, pl.ds(w, 1), at] = jnp.sum(total[q : q + 128].T, axis=0, keepdims=True)

    def across_tiles(h, carry):
        lax.fori_loop(4 * h, 4 * h + 4, receive_other, 0)
        col_half = lax.bitwise_xor(first_half, h)
        row_half = lax.rem(col_half + core, 2)

        def step(i, carry):
            row_at = block(row_half * 8 + i)
            for w in range(WIN_DEV):
                total = rows[w, row_at, :]
                for d in range(8):
                    total = total + pairs(w, row_at, block(col_half * 8 + d), other, other_cols)
                rows[w, row_at, :] = total
                sum_rows(w, row_half * 8 + i, total)
            return carry

        lax.fori_loop(0, 8, step, 0, unroll=UNROLL)
        return carry

    lax.fori_loop(0, 2, across_tiles, 0)

    for i in range(8):
        row_at = block(far + i)
        low = i % 4
        half_at = pl.ds(pl.multiple_of((far + low) * BLOCK + (i // 4) * 128, 128), 128)
        for w in range(WIN_DEV):
            total = rows[w, row_at, :]
            for d in range(4):
                total = total + pairs(w, row_at, block(far + (i + d) % 8), own, own_cols if d else None)
            rows[w, row_at, :] = total
            rows[w, half_at, :] += pairs(w, half_at, block(far + low + 4), own, own_cols)
            if i >= 4:
                sum_rows(w, far + low, rows[w, block(far + low), :])
                sum_rows(w, far + i, rows[w, row_at, :])

    scale = math.sqrt(SPAN) / ASSETS
    for w in range(WIN_DEV):
        one = pl.ds(w, 1)
        result[1, one, :] = jnp.sum(other_cols[w], axis=0, keepdims=True) * scale
        result[0, one, :] = (result[0, one, :] + jnp.sum(own_cols[w], axis=0, keepdims=True)) * scale

    def result_copy(which):
        tile = core if which == 0 else 1 - core
        return pltpu.make_async_remote_copy(
            src_ref=result.at[which],
            dst_ref=arrived.at[which],
            send_sem=result_send.at[which],
            recv_sem=result_recv.at[which],
            device_id=(pair * 2 + half, tile),
            device_id_type=MESH,
        )

    result_copy(1).start()

    @pl.when(core != half)
    def _():
        result_copy(0).start()

    def finish_send(k, carry):
        remote(k).wait_send()
        return carry

    @pl.when(core != half)
    def _():
        remote(0).wait_send()

    lax.fori_loop(1, GROUPS, finish_send, 0)

    def finish_pass(q, carry):
        for w in range(WIN_DEV):
            passing(q, w).wait_send()
        return carry

    lax.fori_loop(0, 8, finish_pass, 0)
    result_copy(1).wait()
    out_ref[1] = arrived[1]

    @pl.when(core != half)
    def _():
        result_copy(0).wait()
        out_ref[0] = arrived[0]

    @pl.when(core == half)
    def _():
        out_ref[0] = result[0]


def shards(tick_bars, prior_bars):
    sums = pl.pallas_call(
        kernel,
        out_shape=jax.ShapeDtypeStruct((2, WIN_DEV, TILE), jnp.float32),
        in_specs=[pl.BlockSpec(memory_space=pl.ANY)] * 2,
        out_specs=pl.BlockSpec(memory_space=pltpu.VMEM),
        scratch_shapes=[
            pltpu.VMEM((SERIES_ROWS, 1, 128), jnp.float32),
            pltpu.VMEM((1, LEAD * GROUP_COLS), jnp.float32),
            pltpu.VMEM((GROUPS, SLOT_ROWS, 1, 128), jnp.float32),
            pltpu.VMEM((2, 4, SLOT_ROWS, 128), jnp.float32),
            pltpu.VMEM((WIN_DEV, 128, TILE), jnp.bfloat16),
            pltpu.VMEM((WIN_DEV, 128, TILE), jnp.bfloat16),
            pltpu.VMEM((TILE, 128), jnp.bfloat16),
            pltpu.VMEM((WIN_DEV, TILE, 128), jnp.float32),
            pltpu.VMEM((WIN_DEV, 8, TILE), jnp.float32),
            pltpu.VMEM((WIN_DEV, 8, TILE), jnp.float32),
            pltpu.VMEM((2, WIN_DEV, TILE), jnp.float32),
            pltpu.VMEM((2, WIN_DEV, TILE), jnp.float32),
            pltpu.SemaphoreType.DMA((2,)),
            pltpu.SemaphoreType.DMA((GROUPS,)),
            pltpu.SemaphoreType.DMA((GROUPS,)),
            pltpu.SemaphoreType.DMA((8, WIN_DEV)),
            pltpu.SemaphoreType.DMA((8, WIN_DEV)),
            pltpu.SemaphoreType.DMA((2,)),
            pltpu.SemaphoreType.DMA((2,)),
        ],
        compiler_params=pltpu.CompilerParams(collective_id=0, has_side_effects=True, vmem_limit_bytes=56 * 2**20),
        name="connect",
    )(tick_bars.reshape(TICK_ROWS, 1, 128), prior_bars.reshape(1, LEAD * GROUP_COLS))
    return sums[0] + sums[1]


def solution(mesh):
    in_specs = (P("asset", "tm", None), P("asset", "tm", None))
    out_specs = P("tm", "asset")
    return jax.shard_map(shards, mesh=mesh, in_specs=in_specs, out_specs=out_specs, check_vma=False)
```

```python
import functools
import math

import jax
import jax.numpy as jnp
from jax import lax
from jax.experimental import pallas as pl
from jax.experimental.pallas import tpu as pltpu
from jax.sharding import PartitionSpec as P

ASSETS = 8192
SPAN = 30
STRIDE = 5
WIN_DEV = 3
LEAD = 25
FLOOR_SQUARES = 1.0

MESH = pl.DeviceIdType.MESH
TILE = ASSETS // 2
GROUPS = 64
GROUP_COLS = TILE // GROUPS
BLOCK_BARS = WIN_DEV * STRIDE
LEAD_ROWS = 13
TICK_ROWS = 480
SERIES_ROWS = LEAD_ROWS + TICK_ROWS + 1
MSG_ROWS = 21
SLOT_ROWS = 24
BLOCK = 256
HALF = TILE // 2
EXT = TILE + HALF
UNROLL = 4


def place():
    tm = lax.axis_index("tm")
    return tm // 2, lax.rem(tm, 2), lax.axis_index("asset")


def magnitudes(lhs, rhs):
    return jnp.abs(
        lax.dot_general(lhs, rhs, (((1,), (0,)), ((), ())), preferred_element_type=jnp.float32)
    )


def fold_rows(a):
    return jnp.sum(a.reshape(a.shape[0] // 8, 8, a.shape[1]), axis=0)


def prepare(raw_ref, bars, ready, turned, chunk, half):
    low = lax.broadcasted_iota(jnp.int32, (SLOT_ROWS, 128), 1) < GROUP_COLS
    valid = lax.broadcasted_iota(jnp.int32, (16, 128), 0) < SPAN // 2
    aligned = half == 1
    for p in range(4):
        slot = chunk * 8 + 2 * p
        a, b = raw_ref[slot, :, 0, :], raw_ref[slot + 1, :, 0, :]
        even = jnp.where(low, a, pltpu.roll(b, GROUP_COLS, 1))
        odd = jnp.where(low, pltpu.roll(a, GROUP_COLS, 1), b)
        bars[0, p] = jnp.where(aligned, even, odd)
        bars[1, p] = jnp.where(aligned, odd, pltpu.roll(even, SLOT_ROWS - 1, 0))
    for p in range(4):
        at = pl.ds(p * 128, 128)
        parts = []
        for w in range(WIN_DEV):
            first = w * STRIDE
            even = jnp.where(valid, bars[0, p, pl.ds((first + 1) // 2, 16), :], 0.0)
            odd = jnp.where(valid, bars[1, p, pl.ds(first // 2, 16), :], 0.0)
            mean = jnp.sum(even + odd, axis=0, keepdims=True) * (1.0 / SPAN)
            even = jnp.where(valid, even - mean, 0.0)
            odd = jnp.where(valid, odd - mean, 0.0)
            squares = jnp.sum(even * even + odd * odd, axis=0, keepdims=True)
            scale = lax.rsqrt(jnp.maximum(squares, FLOOR_SQUARES))
            even, odd = (even * scale).astype(jnp.bfloat16), (odd * scale).astype(jnp.bfloat16)
            ready[w, pl.ds(0, 16), at] = even
            ready[w, pl.ds(16, 16), at] = odd
            parts += [even, odd]
        parts.append(jnp.zeros((32, 128), jnp.bfloat16))
        turned[at, :] = jnp.concatenate(parts, axis=0).T


def settle(ready, turned, scaled, lhs_ref, chunk):
    at = pl.ds(pl.multiple_of(chunk * 512, 512), 512)
    for w in range(WIN_DEV):
        scaled[w, pl.ds(32 * w, 32), at] = ready[w]
    lhs_ref[at, :] = turned[...]


def kernel(
    tick_ref, prior_ref, out_ref, series, prior, own_raw, bars, ready, turned, own, other, lhs_ref, rows, own_cols, other_cols, result, arrived,
    load_sem, send_sem, own_sem, pass_sem, other_sem, result_send, result_recv,
):
    pair, core, half = place()
    me = pair * 2 + core
    sibling = pair * 2 + 1 - core
    prior_load = pltpu.make_async_copy(prior_ref, prior, load_sem.at[0])
    prior_load.start()
    load = pltpu.make_async_copy(tick_ref, series.at[pl.ds(LEAD_ROWS, TICK_ROWS)], load_sem.at[1])
    load.start()

    barrier = pltpu.get_barrier_semaphore()

    def greet(j, carry):
        g = lax.bitwise_xor(me, GROUPS - 1 - j)

        @pl.when(jnp.logical_or(g != me, core != half))
        def _():
            pl.semaphore_signal(barrier, inc=1, device_id=(g, core), device_id_type=MESH)

        return carry

    lax.fori_loop(0, GROUPS, greet, 0)
    pl.semaphore_signal(barrier, inc=1, device_id=(sibling, half), device_id_type=MESH)

    prior_load.wait()
    low = lax.broadcasted_iota(jnp.int32, (1, 128), 1) < GROUP_COLS
    series[0] = jnp.where(low, 0.0, pltpu.roll(prior[:, 0:128], GROUP_COLS, 1))
    for r in range(1, LEAD_ROWS):
        series[r] = prior[:, 128 * r - GROUP_COLS : 128 * r + GROUP_COLS]
    series[LEAD_ROWS + TICK_ROWS] = jnp.zeros((1, 128), jnp.float32)
    own_cols[...] = jnp.zeros_like(own_cols)
    other_cols[...] = jnp.zeros_like(other_cols)

    def clear(i, carry):
        at = pl.ds(pl.multiple_of(i * 256, 256), 256)
        for w in range(WIN_DEV):
            rows[w, at, :] = jnp.zeros((256, 128), jnp.float32)
            for first, last in ((0, 32 * w), (32 * w + 32, 128)):
                if last > first:
                    own[w, pl.ds(first, last - first), at] = jnp.zeros((last - first, 256), jnp.bfloat16)
                    other[w, pl.ds(first, last - first), at] = jnp.zeros((last - first, 256), jnp.bfloat16)
        return carry

    lax.fori_loop(0, TILE // 256, clear, 0)
    pl.semaphore_wait(barrier, GROUPS + jnp.where(core == half, 0, 1))
    load.wait()

    def message(k):
        target_pair = lax.bitwise_xor(pair, k // 2)
        target_half = lax.bitwise_xor(half, lax.rem(k, 2))
        start = (BLOCK_BARS * (2 * target_pair + target_half) + 1) // 2
        return target_pair, target_half, series.at[pl.ds(start, MSG_ROWS)]

    def remote(k):
        target_pair, target_half, src = message(k)
        return pltpu.make_async_remote_copy(
            src_ref=src,
            dst_ref=own_raw.at[me, pl.ds(0, MSG_ROWS)],
            send_sem=send_sem.at[k],
            recv_sem=own_sem.at[me],
            device_id=(target_pair * 2 + half, target_half),
            device_id_type=MESH,
        )

    @pl.when(core == half)
    def _():
        _, _, src = message(0)
        pltpu.make_async_copy(src, own_raw.at[me, pl.ds(0, MSG_ROWS)], own_sem.at[me]).start()

    @pl.when(core != half)
    def _():
        remote(0).start()

    def send(k, carry):
        remote(k).start()
        return carry

    lax.fori_loop(1, GROUPS, send, 0)

    def passing(q, w):
        at = pl.ds(pl.multiple_of(lax.bitwise_xor(me // 8, q) * 512, 512), 512)
        return pltpu.make_async_remote_copy(
            src_ref=own.at[w, pl.ds(32 * w, 32), at],
            dst_ref=other.at[w, pl.ds(32 * w, 32), at],
            send_sem=pass_sem.at[q, w],
            recv_sem=other_sem.at[q, w],
            device_id=(sibling, half),
            device_id_type=MESH,
        )

    def pass_on(q):
        for w in range(WIN_DEV):
            passing(q, w).start()

    def chunk_of(q):
        return lax.bitwise_xor(me // 8, q)

    def receive(q):
        for j in range(8):
            g = chunk_of(q) * 8 + j
            ref = own_raw.at[g, pl.ds(0, MSG_ROWS)]
            pltpu.make_async_copy(ref, ref, own_sem.at[g]).wait()

    def prepare_chunk(q):
        prepare(own_raw, bars, ready, turned, chunk_of(q), half)

    def settle_chunk(q):
        settle(ready, turned, own, lhs_ref, chunk_of(q))

    def block(i):
        return pl.ds(pl.multiple_of(i * BLOCK, BLOCK), BLOCK)

    def pairs(w, row_at, col_at, right, cols):
        a = magnitudes(lhs_ref[row_at, :], right[w, :, col_at])
        if cols is not None:
            cols[w, :, col_at] += fold_rows(a)
        return a[:, :128] + a[:, 128:]

    for q in range(4):
        receive(q)
        prepare_chunk(q)
        settle_chunk(q)
        chunk = chunk_of(q)
        first, second = block(2 * chunk), block(2 * chunk + 1)
        for w in range(WIN_DEV):
            one = pairs(w, first, first, own, None) + pairs(w, first, second, own, own_cols)
            two = pairs(w, second, second, own, None)
            for r in range(q):
                for d in range(2):
                    col_at = block(2 * chunk_of(r) + d)
                    one = one + pairs(w, first, col_at, own, own_cols)
                    two = two + pairs(w, second, col_at, own, own_cols)
            rows[w, first, :] += one
            rows[w, second, :] += two
        pass_on(q)
    first_half = me // 32
    near, far = first_half * 8, 8 - first_half * 8

    def with_near(q, w, i):
        row_at = block(2 * chunk_of(q) + i)
        total = rows[w, row_at, :]
        for d in range(8):
            total = total + pairs(w, row_at, block(near + d), own, own_cols)
        rows[w, row_at, :] = total

    def late(q, carry):
        settle_chunk(q)
        receive(q + 1)
        for i in range(2):
            for w in range(WIN_DEV):
                with_near(q, w, i)
            if i == 0:
                prepare_chunk(q + 1)
        pass_on(q)
        return carry

    receive(4)
    prepare_chunk(4)
    lax.fori_loop(4, 7, late, 0)
    settle_chunk(7)
    pass_on(7)
    for i in range(2):
        for w in range(WIN_DEV):
            with_near(7, w, i)

    def receive_other(q, carry):
        for w in range(WIN_DEV):
            passing(q, w).wait_recv()
        return carry

    def sum_rows(w, i, total):
        for q in range(0, BLOCK, 128):
            at = pl.ds(pl.multiple_of(i * BLOCK + q, 128), 128)
            result[0, pl.ds(w, 1), at] = jnp.sum(total[q : q + 128].T, axis=0, keepdims=True)

    def across_tiles(h, carry):
        lax.fori_loop(4 * h, 4 * h + 4, receive_other, 0)
        col_half = lax.bitwise_xor(first_half, h)
        row_half = lax.rem(col_half + core, 2)

        def step(i, carry):
            row_at = block(row_half * 8 + i)
            for w in range(WIN_DEV):
                total = rows[w, row_at, :]
                for d in range(8):
                    total = total + pairs(w, row_at, block(col_half * 8 + d), other, other_cols)
                rows[w, row_at, :] = total
                sum_rows(w, row_half * 8 + i, total)
            return carry

        lax.fori_loop(0, 8, step, 0, unroll=UNROLL)
        return carry

    lax.fori_loop(0, 2, across_tiles, 0)

    def result_copy(tile, part, which):
        at = pl.ds(pl.multiple_of(part * HALF, HALF), HALF)
        return pltpu.make_async_remote_copy(
            src_ref=result.at[which, :, at],
            dst_ref=arrived.at[which, :, at],
            send_sem=result_send.at[which, part],
            recv_sem=result_recv.at[which, part],
            device_id=(pair * 2 + half, tile),
            device_id_type=MESH,
        )

    scale = math.sqrt(SPAN) / ASSETS

    def sum_columns(part):
        at = pl.ds(pl.multiple_of(part * HALF, HALF), HALF)
        for w in range(WIN_DEV):
            one = pl.ds(w, 1)
            result[0, one, at] = (result[0, one, at] + jnp.sum(own_cols[w, :, at], axis=0, keepdims=True)) * scale

    def send_main(part):
        @pl.when(core != half)
        def _():
            result_copy(core, part, 0).start()

    for w in range(WIN_DEV):
        result[1, pl.ds(w, 1), :] = jnp.sum(other_cols[w], axis=0, keepdims=True) * scale
    sum_columns(first_half)

    def square(h, carry):
        for i in range(4):
            at_block = far + 4 * h + i
            row_at = block(at_block)
            half_at = pl.ds(pl.multiple_of((far + i) * BLOCK + h * 128, 128), 128)
            for w in range(WIN_DEV):
                total = rows[w, row_at, :]
                for d in range(4):
                    col = far + lax.rem(4 * h + i + d, 8)
                    total = total + pairs(w, row_at, block(col), own, own_cols if d else None)
                rows[w, row_at, :] = total
                rows[w, half_at, :] += pairs(w, half_at, block(far + i + 4), own, own_cols)
                sum_rows(w, far + i, rows[w, block(far + i), :])
                sum_rows(w, at_block, rows[w, row_at, :])

        @pl.when(h == 0)
        def _():
            result_copy(1 - core, 0, 1).start()
            result_copy(1 - core, 1, 1).start()
            send_main(first_half)

        return carry

    lax.fori_loop(0, 2, square, 0)
    sum_columns(1 - first_half)
    for part in range(2):
        result_copy(1 - core, part, 1).wait()
    out_ref[1] = arrived[1]
    send_main(1 - first_half)

    def finish_send(k, carry):
        remote(k).wait_send()
        return carry

    @pl.when(core != half)
    def _():
        remote(0).wait_send()

    lax.fori_loop(1, GROUPS, finish_send, 0)

    def finish_pass(q, carry):
        for w in range(WIN_DEV):
            passing(q, w).wait_send()
        return carry

    lax.fori_loop(0, 8, finish_pass, 0)
    @pl.when(core != half)
    def _():
        for part in range(2):
            result_copy(core, part, 0).wait()

    @pl.when(core != half)
    def _():
        out_ref[0] = arrived[0]

    @pl.when(core == half)
    def _():
        out_ref[0] = result[0]


def shards(tick_bars, prior_bars):
    sums = pl.pallas_call(
        kernel,
        out_shape=jax.ShapeDtypeStruct((2, WIN_DEV, TILE), jnp.float32),
        in_specs=[pl.BlockSpec(memory_space=pl.ANY)] * 2,
        out_specs=pl.BlockSpec(memory_space=pltpu.VMEM),
        scratch_shapes=[
            pltpu.VMEM((SERIES_ROWS, 1, 128), jnp.float32),
            pltpu.VMEM((1, LEAD * GROUP_COLS), jnp.float32),
            pltpu.VMEM((GROUPS, SLOT_ROWS, 1, 128), jnp.float32),
            pltpu.VMEM((2, 4, SLOT_ROWS, 128), jnp.float32),
            pltpu.VMEM((WIN_DEV, 32, 512), jnp.bfloat16),
            pltpu.VMEM((512, 128), jnp.bfloat16),
            pltpu.VMEM((WIN_DEV, 128, TILE), jnp.bfloat16),
            pltpu.VMEM((WIN_DEV, 128, TILE), jnp.bfloat16),
            pltpu.VMEM((TILE, 128), jnp.bfloat16),
            pltpu.VMEM((WIN_DEV, TILE, 128), jnp.float32),
            pltpu.VMEM((WIN_DEV, 8, TILE), jnp.float32),
            pltpu.VMEM((WIN_DEV, 8, TILE), jnp.float32),
            pltpu.VMEM((2, WIN_DEV, TILE), jnp.float32),
            pltpu.VMEM((2, WIN_DEV, TILE), jnp.float32),
            pltpu.SemaphoreType.DMA((2,)),
            pltpu.SemaphoreType.DMA((GROUPS,)),
            pltpu.SemaphoreType.DMA((GROUPS,)),
            pltpu.SemaphoreType.DMA((8, WIN_DEV)),
            pltpu.SemaphoreType.DMA((8, WIN_DEV)),
            pltpu.SemaphoreType.DMA((2, 2)),
            pltpu.SemaphoreType.DMA((2, 2)),
        ],
        compiler_params=pltpu.CompilerParams(collective_id=0, has_side_effects=True, vmem_limit_bytes=56 * 2**20),
        name="connect",
    )(tick_bars.reshape(TICK_ROWS, 1, 128), prior_bars.reshape(1, LEAD * GROUP_COLS))
    return sums[0] + sums[1]


def solution(mesh):
    in_specs = (P("asset", "tm", None), P("asset", "tm", None))
    out_specs = P("tm", "asset")
    return jax.shard_map(shards, mesh=mesh, in_specs=in_specs, out_specs=out_specs, check_vma=False)
```

```python
import functools
import math

import jax
import jax.numpy as jnp
from jax import lax
from jax.experimental import pallas as pl
from jax.experimental.pallas import tpu as pltpu
from jax.sharding import PartitionSpec as P

ASSETS = 8192
SPAN = 30
STRIDE = 5
WIN_DEV = 3
LEAD = 25
FLOOR_SQUARES = 1.0

MESH = pl.DeviceIdType.MESH
TILE = ASSETS // 2
GROUPS = 64
GROUP_COLS = TILE // GROUPS
BLOCK_BARS = WIN_DEV * STRIDE
LEAD_ROWS = 13
TICK_ROWS = 480
SERIES_ROWS = LEAD_ROWS + TICK_ROWS + 1
MSG_ROWS = 21
SLOT_ROWS = 24
BLOCK = 256
HALF = TILE // 2


def place():
    tm = lax.axis_index("tm")
    return tm // 2, lax.rem(tm, 2), lax.axis_index("asset")


def magnitudes(lhs, rhs):
    return jnp.abs(
        lax.dot_general(lhs, rhs, (((1,), (0,)), ((), ())), preferred_element_type=jnp.float32)
    )


def fold_rows(a):
    return jnp.sum(a.reshape(a.shape[0] // 8, 8, a.shape[1]), axis=0)


def prepare(raw_ref, bars, ready, turned, chunk, half):
    low = lax.broadcasted_iota(jnp.int32, (SLOT_ROWS, 128), 1) < GROUP_COLS
    valid = lax.broadcasted_iota(jnp.int32, (16, 128), 0) < SPAN // 2
    aligned = half == 1
    for p in range(4):
        slot = chunk * 8 + 2 * p
        a, b = raw_ref[slot, :, 0, :], raw_ref[slot + 1, :, 0, :]
        even = jnp.where(low, a, pltpu.roll(b, GROUP_COLS, 1))
        odd = jnp.where(low, pltpu.roll(a, GROUP_COLS, 1), b)
        bars[0, p] = jnp.where(aligned, even, odd)
        bars[1, p] = jnp.where(aligned, odd, pltpu.roll(even, SLOT_ROWS - 1, 0))
    for p in range(4):
        at = pl.ds(p * 128, 128)
        parts = []
        for w in range(WIN_DEV):
            first = w * STRIDE
            even = jnp.where(valid, bars[0, p, pl.ds((first + 1) // 2, 16), :], 0.0)
            odd = jnp.where(valid, bars[1, p, pl.ds(first // 2, 16), :], 0.0)
            mean = jnp.sum(even + odd, axis=0, keepdims=True) * (1.0 / SPAN)
            even = jnp.where(valid, even - mean, 0.0)
            odd = jnp.where(valid, odd - mean, 0.0)
            squares = jnp.sum(even * even + odd * odd, axis=0, keepdims=True)
            scale = lax.rsqrt(jnp.maximum(squares, FLOOR_SQUARES))
            even, odd = (even * scale).astype(jnp.bfloat16), (odd * scale).astype(jnp.bfloat16)
            ready[w, pl.ds(0, 16), at] = even
            ready[w, pl.ds(16, 16), at] = odd
            parts += [even, odd]
        parts.append(jnp.zeros((32, 128), jnp.bfloat16))
        turned[at, :] = jnp.concatenate(parts, axis=0).T


def settle(ready, turned, scaled, lhs_ref, chunk):
    at = pl.ds(pl.multiple_of(chunk * 512, 512), 512)
    for w in range(WIN_DEV):
        scaled[w, pl.ds(32 * w, 32), at] = ready[w]
    lhs_ref[at, :] = turned[...]


def kernel(
    tick_ref, prior_ref, out_ref, series, prior, own_raw, bars, ready, turned, own, other, lhs_ref, rows, own_cols, other_cols, line, far_sums, near_sums, arrived,
    load_sem, send_sem, own_sem, pass_sem, other_sem, result_send, result_recv,
):
    pair, core, half = place()
    me = pair * 2 + core
    sibling = pair * 2 + 1 - core
    prior_load = pltpu.make_async_copy(prior_ref, prior, load_sem.at[0])
    prior_load.start()
    load = pltpu.make_async_copy(tick_ref, series.at[pl.ds(LEAD_ROWS, TICK_ROWS)], load_sem.at[1])
    load.start()

    barrier = pltpu.get_barrier_semaphore()

    def greet(j, carry):
        k = GROUPS - 1 - j
        target = 2 * lax.bitwise_xor(pair, lax.rem(k, 32)) + core
        pl.semaphore_signal(
            barrier, inc=1, device_id=(target, lax.bitwise_xor(half, k // 32)), device_id_type=MESH
        )
        return carry

    lax.fori_loop(0, GROUPS - 1, greet, 0)
    pl.semaphore_signal(barrier, inc=1, device_id=(sibling, half), device_id_type=MESH)

    @pl.when(core != half)
    def _():
        pl.semaphore_signal(barrier, inc=1, device_id=(sibling, core), device_id_type=MESH)

    prior_load.wait()
    low = lax.broadcasted_iota(jnp.int32, (1, 128), 1) < GROUP_COLS
    series[0] = jnp.where(low, 0.0, pltpu.roll(prior[:, 0:128], GROUP_COLS, 1))
    for r in range(1, LEAD_ROWS):
        series[r] = prior[:, 128 * r - GROUP_COLS : 128 * r + GROUP_COLS]
    series[LEAD_ROWS + TICK_ROWS] = jnp.zeros((1, 128), jnp.float32)
    own_cols[...] = jnp.zeros_like(own_cols)
    other_cols[...] = jnp.zeros_like(other_cols)

    def clear(i, carry):
        at = pl.ds(pl.multiple_of(i * 256, 256), 256)
        for w in range(WIN_DEV):
            rows[w, at, :] = jnp.zeros((256, 128), jnp.float32)
            for first, last in ((0, 32 * w), (32 * w + 32, 128)):
                if last > first:
                    own[w, pl.ds(first, last - first), at] = jnp.zeros((last - first, 256), jnp.bfloat16)
                    other[w, pl.ds(first, last - first), at] = jnp.zeros((last - first, 256), jnp.bfloat16)
        return carry

    lax.fori_loop(0, TILE // 256, clear, 0)
    pl.semaphore_wait(barrier, GROUPS + jnp.where(core == half, 0, 1))
    load.wait()

    my_slot = half * 32 + pair

    def message(k):
        target_pair = lax.bitwise_xor(pair, lax.rem(k, 32))
        target_half = lax.bitwise_xor(half, k // 32)
        start = (BLOCK_BARS * (2 * target_pair + target_half) + 1) // 2
        return target_pair, target_half, series.at[pl.ds(start, MSG_ROWS)]

    def remote(k):
        target_pair, target_half, src = message(k)
        return pltpu.make_async_remote_copy(
            src_ref=src,
            dst_ref=own_raw.at[my_slot, pl.ds(0, MSG_ROWS)],
            send_sem=send_sem,
            recv_sem=own_sem.at[my_slot // 8],
            device_id=(target_pair * 2 + core, target_half),
            device_id_type=MESH,
        )

    def send(k, carry):
        remote(k).start()
        return carry

    lax.fori_loop(1, GROUPS, send, 0)
    _, _, kept = message(0)
    pltpu.make_async_copy(kept, own_raw.at[my_slot, pl.ds(0, MSG_ROWS)], own_sem.at[my_slot // 8]).start()

    def chunk_of(q):
        return lax.bitwise_xor(my_slot // 8, q)

    def passing(q, w):
        at = pl.ds(pl.multiple_of(chunk_of(q) * 512, 512), 512)
        return pltpu.make_async_remote_copy(
            src_ref=own.at[w, pl.ds(32 * w, 32), at],
            dst_ref=other.at[w, pl.ds(32 * w, 32), at],
            send_sem=pass_sem.at[q, w],
            recv_sem=other_sem.at[q, w],
            device_id=(sibling, half),
            device_id_type=MESH,
        )

    def pass_on(q):
        for w in range(WIN_DEV):
            passing(q, w).start()

    def receive(q):
        ref = own_raw.at[pl.ds(chunk_of(q) * 8, 8), pl.ds(0, MSG_ROWS)]
        pltpu.make_async_copy(ref, ref, own_sem.at[chunk_of(q)]).wait()

    def prepare_chunk(q):
        prepare(own_raw, bars, ready, turned, chunk_of(q), half)

    def settle_chunk(q):
        settle(ready, turned, own, lhs_ref, chunk_of(q))

    def block(i):
        return pl.ds(pl.multiple_of(i * BLOCK, BLOCK), BLOCK)

    def pairs(w, row_at, col_at, right, cols):
        a = magnitudes(lhs_ref[row_at, :], right[w, :, col_at])
        if cols is not None:
            cols[w, :, col_at] += fold_rows(a)
        return a[:, :128] + a[:, 128:]

    for q in range(4):
        receive(q)
        prepare_chunk(q)
        settle_chunk(q)
        chunk = chunk_of(q)
        first, second = block(2 * chunk), block(2 * chunk + 1)
        for w in range(WIN_DEV):
            one = pairs(w, first, first, own, None) + pairs(w, first, second, own, own_cols)
            two = pairs(w, second, second, own, None)
            for r in range(q):
                for d in range(2):
                    col_at = block(2 * chunk_of(r) + d)
                    one = one + pairs(w, first, col_at, own, own_cols)
                    two = two + pairs(w, second, col_at, own, own_cols)
            rows[w, first, :] += one
            rows[w, second, :] += two
        pass_on(q)
    near, far = half * 8, 8 - half * 8

    def with_near(q, w, i):
        row_at = block(2 * chunk_of(q) + i)
        total = rows[w, row_at, :]
        for d in range(8):
            total = total + pairs(w, row_at, block(near + d), own, own_cols)
        rows[w, row_at, :] = total

    def late(q, carry):
        settle_chunk(q)
        for w in range(WIN_DEV):
            with_near(q, w, 0)
        pass_on(q)
        receive(q + 1)
        prepare_chunk(q + 1)
        for w in range(WIN_DEV):
            with_near(q, w, 1)
        return carry

    receive(4)
    prepare_chunk(4)
    lax.fori_loop(4, 7, late, 0)
    settle_chunk(7)
    pass_on(7)
    for i in range(2):
        for w in range(WIN_DEV):
            with_near(7, w, i)

    def square(h, carry):
        for i in range(4):
            row_at = block(far + 4 * h + i)
            half_at = pl.ds(pl.multiple_of((far + i) * BLOCK + h * 128, 128), 128)
            for w in range(WIN_DEV):
                total = rows[w, row_at, :]
                for d in range(4):
                    col = far + lax.rem(4 * h + i + d, 8)
                    total = total + pairs(w, row_at, block(col), own, own_cols if d else None)
                rows[w, row_at, :] = total
                rows[w, half_at, :] += pairs(w, half_at, block(far + i + 4), own, own_cols)
        return carry

    lax.fori_loop(0, 2, square, 0)

    def finish_pass(q, carry):
        for w in range(WIN_DEV):
            passing(q, w).wait_send()
        return carry

    def receive_other(q, carry):
        for w in range(WIN_DEV):
            passing(q, w).wait_recv()
        return carry

    lax.fori_loop(0, 8, receive_other, 0)

    scale = math.sqrt(SPAN) / ASSETS

    def gather_sums(first_block, sums):
        at = pl.ds(pl.multiple_of(first_block * BLOCK, BLOCK), HALF)
        for w in range(WIN_DEV):
            one = pl.ds(w, 1)
            sums[core, one, :] = (line[one, at] + jnp.sum(own_cols[w, :, at], axis=0, keepdims=True)) * scale
            sums[1 - core, one, :] = jnp.sum(other_cols[w, :, at], axis=0, keepdims=True) * scale

    far_copy = pltpu.make_async_remote_copy(
        src_ref=far_sums,
        dst_ref=arrived.at[core],
        send_sem=result_send.at[0],
        recv_sem=result_recv.at[core],
        device_id=(pair * 2 + half, 1 - half),
        device_id_type=MESH,
    )
    near_copy = pltpu.make_async_remote_copy(
        src_ref=near_sums,
        dst_ref=arrived.at[core],
        send_sem=result_send.at[1],
        recv_sem=result_recv.at[core],
        device_id=(sibling, half),
        device_id_type=MESH,
    )

    def across(part, carry):
        row_first = jnp.where(lax.rem(part, 2) == 0, far, near)
        col_first = jnp.where(part < 2, far, near)
        for t in range(2):
            cols_from = col_first + 4 * lax.rem(t + core, 2)
            for i in range(4):
                at_block = row_first + 4 * t + i
                row_at = block(at_block)
                for w in range(WIN_DEV):
                    total = rows[w, row_at, :]
                    for d in range(4):
                        total = total + pairs(w, row_at, block(cols_from + d), other, other_cols)
                    rows[w, row_at, :] = total
                    for p in range(0, BLOCK, 128):
                        at = pl.ds(pl.multiple_of(at_block * BLOCK + p, 128), 128)
                        line[pl.ds(w, 1), at] = jnp.sum(total[p : p + 128].T, axis=0, keepdims=True)

        @pl.when(part == 2)
        def _():
            gather_sums(far, far_sums)

            sent = own_raw.at[pl.ds(0, GROUPS - 1), pl.ds(0, MSG_ROWS)]
            pltpu.make_async_copy(sent, sent, send_sem).wait()
            lax.fori_loop(0, 8, finish_pass, 0)
            far_copy.start()

        return carry

    lax.fori_loop(0, 4, across, 0)
    gather_sums(near, near_sums)

    lanes_low = lax.broadcasted_iota(jnp.int32, (WIN_DEV, 128), 1) < GROUP_COLS

    def write_out(first, second):
        for p in range(HALF // 128):
            at = pl.ds(p * 128, 128)
            zero = first[0, :, at] + second[0, :, at]
            one = first[1, :, at] + second[1, :, at]
            out_ref[:, pl.ds(2 * p * 128, 128)] = jnp.where(lanes_low, zero, pltpu.roll(one, GROUP_COLS, 1))
            out_ref[:, pl.ds((2 * p + 1) * 128, 128)] = jnp.where(lanes_low, pltpu.roll(zero, GROUP_COLS, 1), one)

    @pl.when(core != half)
    def _():
        near_copy.start()
        for d in range(2):
            pltpu.make_async_copy(arrived.at[d], arrived.at[d], result_recv.at[d]).wait()
        write_out(arrived.at[0], arrived.at[1])
        near_copy.wait_send()

    @pl.when(core == half)
    def _():
        other_core = 1 - core
        pltpu.make_async_copy(arrived.at[other_core], arrived.at[other_core], result_recv.at[other_core]).wait()
        write_out(near_sums, arrived.at[other_core])

    far_copy.wait_send()


def shards(tick_bars, prior_bars):
    return pl.pallas_call(
        kernel,
        out_shape=jax.ShapeDtypeStruct((WIN_DEV, TILE), jnp.float32),
        in_specs=[pl.BlockSpec(memory_space=pl.ANY)] * 2,
        out_specs=pl.BlockSpec(memory_space=pltpu.VMEM),
        scratch_shapes=[
            pltpu.VMEM((SERIES_ROWS, 1, 128), jnp.float32),
            pltpu.VMEM((1, LEAD * GROUP_COLS), jnp.float32),
            pltpu.VMEM((GROUPS, SLOT_ROWS, 1, 128), jnp.float32),
            pltpu.VMEM((2, 4, SLOT_ROWS, 128), jnp.float32),
            pltpu.VMEM((WIN_DEV, 32, 512), jnp.bfloat16),
            pltpu.VMEM((512, 128), jnp.bfloat16),
            pltpu.VMEM((WIN_DEV, 128, TILE), jnp.bfloat16),
            pltpu.VMEM((WIN_DEV, 128, TILE), jnp.bfloat16),
            pltpu.VMEM((TILE, 128), jnp.bfloat16),
            pltpu.VMEM((WIN_DEV, TILE, 128), jnp.float32),
            pltpu.VMEM((WIN_DEV, 8, TILE), jnp.float32),
            pltpu.VMEM((WIN_DEV, 8, TILE), jnp.float32),
            pltpu.VMEM((WIN_DEV, TILE), jnp.float32),
            pltpu.VMEM((2, WIN_DEV, HALF), jnp.float32),
            pltpu.VMEM((2, WIN_DEV, HALF), jnp.float32),
            pltpu.VMEM((2, 2, WIN_DEV, HALF), jnp.float32),
            pltpu.SemaphoreType.DMA((2,)),
            pltpu.SemaphoreType.DMA,
            pltpu.SemaphoreType.DMA((8,)),
            pltpu.SemaphoreType.DMA((8, WIN_DEV)),
            pltpu.SemaphoreType.DMA((8, WIN_DEV)),
            pltpu.SemaphoreType.DMA((2,)),
            pltpu.SemaphoreType.DMA((2,)),
        ],
        compiler_params=pltpu.CompilerParams(collective_id=0, has_side_effects=True, vmem_limit_bytes=56 * 2**20),
        name="connect",
    )(tick_bars.reshape(TICK_ROWS, 1, 128), prior_bars.reshape(1, LEAD * GROUP_COLS))


def solution(mesh):
    in_specs = (P("asset", "tm", None), P("asset", "tm", None))
    out_specs = P("tm", "asset")
    return jax.shard_map(shards, mesh=mesh, in_specs=in_specs, out_specs=out_specs, check_vma=False)
```

```python
import functools
import math

import jax
import jax.numpy as jnp
from jax import lax
from jax.experimental import pallas as pl
from jax.experimental.pallas import tpu as pltpu
from jax.sharding import PartitionSpec as P

ASSETS = 8192
SPAN = 30
STRIDE = 5
WIN_DEV = 3
LEAD = 25
FLOOR_SQUARES = 1.0

MESH = pl.DeviceIdType.MESH
TILE = ASSETS // 2
GROUPS = 64
GROUP_COLS = TILE // GROUPS
BLOCK_BARS = WIN_DEV * STRIDE
FIRST_ROW = 3
TICK_FIRST = 16
TICK_ROWS = 480
SERIES_ROWS = TICK_FIRST + TICK_ROWS + 8
PIECES = 5
FAR_AFTER = 0
BLOCK = 256
HALF = TILE // 2


def place():
    tm = lax.axis_index("tm")
    return tm // 2, lax.rem(tm, 2), lax.axis_index("asset")


def magnitudes(lhs, rhs):
    return jnp.abs(
        lax.dot_general(lhs, rhs, (((1,), (0,)), ((), ())), preferred_element_type=jnp.float32)
    )


def fold_rows(a):
    return jnp.sum(a.reshape(a.shape[0] // 8, 8, a.shape[1]), axis=0)


def prepare(raw_ref, bars, ready, turned, chunk):
    low = lax.broadcasted_iota(jnp.int32, (4, 128), 1) < GROUP_COLS
    valid = lax.broadcasted_iota(jnp.int32, (16, 128), 0) < SPAN // 2
    for p in range(4):
        slot = chunk * 8 + 2 * p
        for j in range(PIECES):
            a, b = raw_ref[slot, j], raw_ref[slot + 1, j]
            bars[0, p, pl.ds(4 * j, 4), :] = jnp.where(low, a, pltpu.roll(b, GROUP_COLS, 1))
            bars[1, p, pl.ds(4 * j, 4), :] = jnp.where(low, pltpu.roll(a, GROUP_COLS, 1), b)
    for p in range(4):
        at = pl.ds(p * 128, 128)
        parts = []
        for w in range(WIN_DEV):
            first = w * STRIDE
            even = jnp.where(valid, bars[0, p, pl.ds((first + 1) // 2, 16), :], 0.0)
            odd = jnp.where(valid, bars[1, p, pl.ds(first // 2, 16), :], 0.0)
            mean = jnp.sum(even + odd, axis=0, keepdims=True) * (1.0 / SPAN)
            even = jnp.where(valid, even - mean, 0.0)
            odd = jnp.where(valid, odd - mean, 0.0)
            squares = jnp.sum(even * even + odd * odd, axis=0, keepdims=True)
            scale = lax.rsqrt(jnp.maximum(squares, FLOOR_SQUARES))
            even, odd = (even * scale).astype(jnp.bfloat16), (odd * scale).astype(jnp.bfloat16)
            ready[w, pl.ds(0, 16), at] = even
            ready[w, pl.ds(16, 16), at] = odd
            parts += [even, odd]
        parts.append(jnp.zeros((32, 128), jnp.bfloat16))
        turned[at, :] = jnp.concatenate(parts, axis=0).T


def settle(ready, turned, scaled, lhs_ref, chunk):
    at = pl.ds(pl.multiple_of(chunk * 512, 512), 512)
    for w in range(WIN_DEV):
        scaled[w, pl.ds(32 * w, 32), at] = ready[w]
    lhs_ref[at, :] = turned[...]


def kernel(
    tick_ref, prior_ref, out_ref, series, prior, messages, own_raw, bars, ready, turned, own, other, lhs_ref, rows, own_cols, other_cols, line, far_sums, near_sums, arrived,
    load_sem, send_sem, own_sem, pass_sem, other_sem, result_send, result_recv,
):
    pair, core, half = place()
    me = pair * 2 + core
    sibling = pair * 2 + 1 - core
    prior_load = pltpu.make_async_copy(prior_ref, prior, load_sem.at[0])
    prior_load.start()
    load = pltpu.make_async_copy(tick_ref, series.at[pl.ds(TICK_FIRST, TICK_ROWS)], load_sem.at[1])
    load.start()

    barrier = pltpu.get_barrier_semaphore()

    def greet(j, carry):
        k = GROUPS - 1 - j
        target = 2 * lax.bitwise_xor(pair, lax.rem(k, 32)) + core
        pl.semaphore_signal(
            barrier, inc=1, device_id=(target, lax.bitwise_xor(half, k // 32)), device_id_type=MESH
        )
        return carry

    lax.fori_loop(0, GROUPS - 1, greet, 0)
    pl.semaphore_signal(barrier, inc=1, device_id=(sibling, half), device_id_type=MESH)

    @pl.when(core != half)
    def _():
        pl.semaphore_signal(barrier, inc=1, device_id=(sibling, core), device_id_type=MESH)

    prior_load.wait()
    low = lax.broadcasted_iota(jnp.int32, (1, 128), 1) < GROUP_COLS
    series[pl.ds(FIRST_ROW, 1), :] = jnp.where(low, 0.0, pltpu.roll(prior[:, 0:128], GROUP_COLS, 1))
    for r in range(1, TICK_FIRST - FIRST_ROW):
        series[pl.ds(FIRST_ROW + r, 1), :] = prior[:, 128 * r - GROUP_COLS : 128 * r + GROUP_COLS]
    series[pl.ds(TICK_FIRST + TICK_ROWS, 8), :] = jnp.zeros((8, 128), jnp.float32)
    load.wait()

    lows = lax.broadcasted_iota(jnp.int32, (4, 128), 1) < GROUP_COLS

    def assemble(t, carry):
        even = FIRST_ROW + BLOCK_BARS * t
        odd = FIRST_ROW + BLOCK_BARS * t + 8
        for j in range(PIECES):
            here, after = series[pl.ds(even + 4 * j, 4), :], series[pl.ds(even + 4 * j + 1, 4), :]
            messages[t, j] = pltpu.roll(jnp.where(lows, after, here), GROUP_COLS, 1)
            messages[32 + t, j] = series[pl.ds(odd + 4 * j, 4), :]
        return carry

    lax.fori_loop(0, 32, assemble, 0, unroll=2)
    own_cols[...] = jnp.zeros_like(own_cols)
    other_cols[...] = jnp.zeros_like(other_cols)

    def clear(i, carry):
        at = pl.ds(pl.multiple_of(i * 256, 256), 256)
        for w in range(WIN_DEV):
            rows[w, at, :] = jnp.zeros((256, 128), jnp.float32)
            for first, last in ((0, 32 * w), (32 * w + 32, 128)):
                if last > first:
                    own[w, pl.ds(first, last - first), at] = jnp.zeros((last - first, 256), jnp.bfloat16)
                    other[w, pl.ds(first, last - first), at] = jnp.zeros((last - first, 256), jnp.bfloat16)
        return carry

    lax.fori_loop(0, TILE // 256, clear, 0)
    pl.semaphore_wait(barrier, GROUPS + jnp.where(core == half, 0, 1))

    my_slot = half * 32 + pair

    def message(k):
        target_pair = lax.bitwise_xor(pair, lax.rem(k, 32))
        target_half = lax.bitwise_xor(half, k // 32)
        return target_pair, target_half, messages.at[target_half * 32 + target_pair]

    def remote(k):
        target_pair, target_half, src = message(k)
        return pltpu.make_async_remote_copy(
            src_ref=src,
            dst_ref=own_raw.at[my_slot],
            send_sem=send_sem,
            recv_sem=own_sem.at[my_slot // 8],
            device_id=(target_pair * 2 + core, target_half),
            device_id_type=MESH,
        )

    def send(k, carry):
        remote(k).start()
        return carry

    lax.fori_loop(1, 32, send, 0)
    _, _, kept = message(0)
    pltpu.make_async_copy(kept, own_raw.at[my_slot], own_sem.at[my_slot // 8]).start()

    def chunk_of(q):
        return lax.bitwise_xor(my_slot // 8, q)

    def passing(q, w):
        at = pl.ds(pl.multiple_of(chunk_of(q) * 512, 512), 512)
        return pltpu.make_async_remote_copy(
            src_ref=own.at[w, pl.ds(32 * w, 32), at],
            dst_ref=other.at[w, pl.ds(32 * w, 32), at],
            send_sem=pass_sem.at[q, w],
            recv_sem=other_sem.at[q, w],
            device_id=(sibling, half),
            device_id_type=MESH,
        )

    def pass_on(q):
        for w in range(WIN_DEV):
            passing(q, w).start()

    def receive(q):
        ref = own_raw.at[pl.ds(chunk_of(q) * 8, 8)]
        pltpu.make_async_copy(ref, ref, own_sem.at[chunk_of(q)]).wait()

    def prepare_chunk(q):
        prepare(own_raw, bars, ready, turned, chunk_of(q))

    def settle_chunk(q):
        settle(ready, turned, own, lhs_ref, chunk_of(q))

    def block(i):
        return pl.ds(pl.multiple_of(i * BLOCK, BLOCK), BLOCK)

    def pairs(w, row_at, col_at, right, cols):
        a = magnitudes(lhs_ref[row_at, :], right[w, :, col_at])
        if cols is not None:
            cols[w, :, col_at] += fold_rows(a)
        return a[:, :128] + a[:, 128:]

    if FAR_AFTER < 0:
        lax.fori_loop(32, GROUPS, send, 0)
    for q in range(4):
        receive(q)
        if q == FAR_AFTER:
            lax.fori_loop(32, GROUPS, send, 0)
        prepare_chunk(q)
        settle_chunk(q)
        chunk = chunk_of(q)
        first, second = block(2 * chunk), block(2 * chunk + 1)
        for w in range(WIN_DEV):
            one = pairs(w, first, first, own, None) + pairs(w, first, second, own, own_cols)
            two = pairs(w, second, second, own, None)
            for r in range(q):
                for d in range(2):
                    col_at = block(2 * chunk_of(r) + d)
                    one = one + pairs(w, first, col_at, own, own_cols)
                    two = two + pairs(w, second, col_at, own, own_cols)
            rows[w, first, :] += one
            rows[w, second, :] += two
        pass_on(q)
    near, far = half * 8, 8 - half * 8

    def with_near(q, w, i):
        row_at = block(2 * chunk_of(q) + i)
        total = rows[w, row_at, :]
        for d in range(8):
            total = total + pairs(w, row_at, block(near + d), own, own_cols)
        rows[w, row_at, :] = total

    def late(q, carry):
        settle_chunk(q)
        for w in range(WIN_DEV):
            with_near(q, w, 0)
        pass_on(q)
        receive(q + 1)
        prepare_chunk(q + 1)
        for w in range(WIN_DEV):
            with_near(q, w, 1)
        return carry

    receive(4)
    prepare_chunk(4)
    lax.fori_loop(4, 7, late, 0)
    settle_chunk(7)
    pass_on(7)
    for i in range(2):
        for w in range(WIN_DEV):
            with_near(7, w, i)

    def square(h, carry):
        for i in range(4):
            row_at = block(far + 4 * h + i)
            half_at = pl.ds(pl.multiple_of((far + i) * BLOCK + h * 128, 128), 128)
            for w in range(WIN_DEV):
                total = rows[w, row_at, :]
                for d in range(4):
                    col = far + lax.rem(4 * h + i + d, 8)
                    total = total + pairs(w, row_at, block(col), own, own_cols if d else None)
                rows[w, row_at, :] = total
                rows[w, half_at, :] += pairs(w, half_at, block(far + i + 4), own, own_cols)
        return carry

    lax.fori_loop(0, 2, square, 0)

    def finish_pass(q, carry):
        for w in range(WIN_DEV):
            passing(q, w).wait_send()
        return carry

    def receive_other(q, carry):
        for w in range(WIN_DEV):
            passing(q, w).wait_recv()
        return carry

    lax.fori_loop(0, 8, receive_other, 0)

    scale = math.sqrt(SPAN) / ASSETS

    def gather_sums(first_block, sums):
        at = pl.ds(pl.multiple_of(first_block * BLOCK, BLOCK), HALF)
        for w in range(WIN_DEV):
            one = pl.ds(w, 1)
            sums[core, one, :] = (line[one, at] + jnp.sum(own_cols[w, :, at], axis=0, keepdims=True)) * scale
            sums[1 - core, one, :] = jnp.sum(other_cols[w, :, at], axis=0, keepdims=True) * scale

    far_copy = pltpu.make_async_remote_copy(
        src_ref=far_sums,
        dst_ref=arrived.at[core],
        send_sem=result_send.at[0],
        recv_sem=result_recv.at[core],
        device_id=(pair * 2 + half, 1 - half),
        device_id_type=MESH,
    )
    near_copy = pltpu.make_async_remote_copy(
        src_ref=near_sums,
        dst_ref=arrived.at[core],
        send_sem=result_send.at[1],
        recv_sem=result_recv.at[core],
        device_id=(sibling, half),
        device_id_type=MESH,
    )

    def across(part, carry):
        row_first = jnp.where(lax.rem(part, 2) == 0, far, near)
        col_first = jnp.where(part < 2, far, near)
        for t in range(2):
            cols_from = col_first + 4 * lax.rem(t + core, 2)
            for i in range(4):
                at_block = row_first + 4 * t + i
                row_at = block(at_block)
                for w in range(WIN_DEV):
                    total = rows[w, row_at, :]
                    for d in range(4):
                        total = total + pairs(w, row_at, block(cols_from + d), other, other_cols)
                    rows[w, row_at, :] = total
                    for p in range(0, BLOCK, 128):
                        at = pl.ds(pl.multiple_of(at_block * BLOCK + p, 128), 128)
                        line[pl.ds(w, 1), at] = jnp.sum(total[p : p + 128].T, axis=0, keepdims=True)

        @pl.when(part == 2)
        def _():
            gather_sums(far, far_sums)

            sent = own_raw.at[pl.ds(0, GROUPS - 1)]
            pltpu.make_async_copy(sent, sent, send_sem).wait()
            lax.fori_loop(0, 8, finish_pass, 0)
            far_copy.start()

        return carry

    lax.fori_loop(0, 4, across, 0)
    gather_sums(near, near_sums)

    lanes_low = lax.broadcasted_iota(jnp.int32, (WIN_DEV, 128), 1) < GROUP_COLS

    def write_out(first, second):
        for p in range(HALF // 128):
            at = pl.ds(p * 128, 128)
            zero = first[0, :, at] + second[0, :, at]
            one = first[1, :, at] + second[1, :, at]
            out_ref[:, pl.ds(2 * p * 128, 128)] = jnp.where(lanes_low, zero, pltpu.roll(one, GROUP_COLS, 1))
            out_ref[:, pl.ds((2 * p + 1) * 128, 128)] = jnp.where(lanes_low, pltpu.roll(zero, GROUP_COLS, 1), one)

    @pl.when(core != half)
    def _():
        near_copy.start()
        for d in range(2):
            pltpu.make_async_copy(arrived.at[d], arrived.at[d], result_recv.at[d]).wait()
        write_out(arrived.at[0], arrived.at[1])
        near_copy.wait_send()

    @pl.when(core == half)
    def _():
        other_core = 1 - core
        pltpu.make_async_copy(arrived.at[other_core], arrived.at[other_core], result_recv.at[other_core]).wait()
        write_out(near_sums, arrived.at[other_core])

    far_copy.wait_send()


def shards(tick_bars, prior_bars):
    return pl.pallas_call(
        kernel,
        out_shape=jax.ShapeDtypeStruct((WIN_DEV, TILE), jnp.float32),
        in_specs=[pl.BlockSpec(memory_space=pl.ANY)] * 2,
        out_specs=pl.BlockSpec(memory_space=pltpu.VMEM),
        scratch_shapes=[
            pltpu.VMEM((SERIES_ROWS, 128), jnp.float32),
            pltpu.VMEM((1, LEAD * GROUP_COLS), jnp.float32),
            pltpu.VMEM((GROUPS, PIECES, 4, 128), jnp.float32),
            pltpu.VMEM((GROUPS, PIECES, 4, 128), jnp.float32),
            pltpu.VMEM((2, 4, 24, 128), jnp.float32),
            pltpu.VMEM((WIN_DEV, 32, 512), jnp.bfloat16),
            pltpu.VMEM((512, 128), jnp.bfloat16),
            pltpu.VMEM((WIN_DEV, 128, TILE), jnp.bfloat16),
            pltpu.VMEM((WIN_DEV, 128, TILE), jnp.bfloat16),
            pltpu.VMEM((TILE, 128), jnp.bfloat16),
            pltpu.VMEM((WIN_DEV, TILE, 128), jnp.float32),
            pltpu.VMEM((WIN_DEV, 8, TILE), jnp.float32),
            pltpu.VMEM((WIN_DEV, 8, TILE), jnp.float32),
            pltpu.VMEM((WIN_DEV, TILE), jnp.float32),
            pltpu.VMEM((2, WIN_DEV, HALF), jnp.float32),
            pltpu.VMEM((2, WIN_DEV, HALF), jnp.float32),
            pltpu.VMEM((2, 2, WIN_DEV, HALF), jnp.float32),
            pltpu.SemaphoreType.DMA((2,)),
            pltpu.SemaphoreType.DMA,
            pltpu.SemaphoreType.DMA((8,)),
            pltpu.SemaphoreType.DMA((8, WIN_DEV)),
            pltpu.SemaphoreType.DMA((8, WIN_DEV)),
            pltpu.SemaphoreType.DMA((2,)),
            pltpu.SemaphoreType.DMA((2,)),
        ],
        compiler_params=pltpu.CompilerParams(collective_id=0, has_side_effects=True, vmem_limit_bytes=56 * 2**20),
        name="connect",
    )(tick_bars.reshape(TICK_ROWS, 128), prior_bars.reshape(1, LEAD * GROUP_COLS))


def solution(mesh):
    in_specs = (P("asset", "tm", None), P("asset", "tm", None))
    out_specs = P("tm", "asset")
    return jax.shard_map(shards, mesh=mesh, in_specs=in_specs, out_specs=out_specs, check_vma=False)
```

```python
import functools
import math

import jax
import jax.numpy as jnp
from jax import lax
from jax.experimental import pallas as pl
from jax.experimental.pallas import tpu as pltpu
from jax.sharding import PartitionSpec as P

ASSETS = 8192
SPAN = 30
STRIDE = 5
WIN_DEV = 3
LEAD = 25
FLOOR_SQUARES = 1.0

MESH = pl.DeviceIdType.MESH
TILE = ASSETS // 2
GROUPS = 64
GROUP_COLS = TILE // GROUPS
BLOCK_BARS = WIN_DEV * STRIDE
FIRST_ROW = 3
TICK_FIRST = 16
TICK_ROWS = 480
SERIES_ROWS = TICK_FIRST + TICK_ROWS + 8
PIECES = 5
BLOCK = 256
HALF = TILE // 2


def place():
    tm = lax.axis_index("tm")
    return tm // 2, lax.rem(tm, 2), lax.axis_index("asset")


def magnitudes(lhs, rhs):
    return jnp.abs(
        lax.dot_general(lhs, rhs, (((1,), (0,)), ((), ())), preferred_element_type=jnp.float32)
    )


def fold_rows(a):
    return jnp.sum(a.reshape(a.shape[0] // 8, 8, a.shape[1]), axis=0)


def prepare(raw_ref, bars, ready, turned, chunk):
    low = lax.broadcasted_iota(jnp.int32, (4, 128), 1) < GROUP_COLS
    valid = lax.broadcasted_iota(jnp.int32, (16, 128), 0) < SPAN // 2
    for p in range(4):
        slot = chunk * 8 + 2 * p
        for j in range(PIECES):
            a, b = raw_ref[slot, j], raw_ref[slot + 1, j]
            bars[0, p, pl.ds(4 * j, 4), :] = jnp.where(low, a, pltpu.roll(b, GROUP_COLS, 1))
            bars[1, p, pl.ds(4 * j, 4), :] = jnp.where(low, pltpu.roll(a, GROUP_COLS, 1), b)
    for p in range(4):
        at = pl.ds(p * 128, 128)
        parts = []
        for w in range(WIN_DEV):
            first = w * STRIDE
            even = jnp.where(valid, bars[0, p, pl.ds((first + 1) // 2, 16), :], 0.0)
            odd = jnp.where(valid, bars[1, p, pl.ds(first // 2, 16), :], 0.0)
            mean = jnp.sum(even + odd, axis=0, keepdims=True) * (1.0 / SPAN)
            even = jnp.where(valid, even - mean, 0.0)
            odd = jnp.where(valid, odd - mean, 0.0)
            squares = jnp.sum(even * even + odd * odd, axis=0, keepdims=True)
            scale = lax.rsqrt(jnp.maximum(squares, FLOOR_SQUARES))
            even, odd = (even * scale).astype(jnp.bfloat16), (odd * scale).astype(jnp.bfloat16)
            ready[w, pl.ds(0, 16), at] = even
            ready[w, pl.ds(16, 16), at] = odd
            parts += [even, odd]
        parts.append(jnp.zeros((32, 128), jnp.bfloat16))
        turned[at, :] = jnp.concatenate(parts, axis=0).T


def settle(ready, turned, scaled, lhs_ref, chunk):
    at = pl.ds(pl.multiple_of(chunk * 512, 512), 512)
    for w in range(WIN_DEV):
        scaled[w, pl.ds(32 * w, 32), at] = ready[w]
    lhs_ref[at, :] = turned[...]


def kernel(
    tick_ref, prior_ref, out_ref, series, prior, messages, own_raw, bars, ready, turned, own, other, lhs_ref, rows, own_cols, other_cols, line, far_sums, near_sums, arrived,
    load_sem, send_sem, own_sem, pass_sem, other_sem, result_send, result_recv, far_ready,
):
    pair, core, half = place()
    me = pair * 2 + core
    sibling = pair * 2 + 1 - core
    prior_load = pltpu.make_async_copy(prior_ref, prior, load_sem.at[0])
    prior_load.start()
    load = pltpu.make_async_copy(tick_ref, series.at[pl.ds(TICK_FIRST, TICK_ROWS)], load_sem.at[1])
    load.start()

    barrier = pltpu.get_barrier_semaphore()

    def greet(j, carry):
        target = 2 * lax.bitwise_xor(pair, 31 - j) + core
        pl.semaphore_signal(barrier, inc=1, device_id=(target, half), device_id_type=MESH)
        return carry

    lax.fori_loop(0, 31, greet, 0)
    pl.semaphore_signal(barrier, inc=1, device_id=(sibling, half), device_id_type=MESH)
    pl.semaphore_signal(barrier, inc=1, device_id=(me, 1 - half), device_id_type=MESH)

    @pl.when(core != half)
    def _():
        pl.semaphore_signal(barrier, inc=1, device_id=(sibling, core), device_id_type=MESH)

    prior_load.wait()
    low = lax.broadcasted_iota(jnp.int32, (1, 128), 1) < GROUP_COLS
    series[pl.ds(FIRST_ROW, 1), :] = jnp.where(low, 0.0, pltpu.roll(prior[:, 0:128], GROUP_COLS, 1))
    for r in range(1, TICK_FIRST - FIRST_ROW):
        series[pl.ds(FIRST_ROW + r, 1), :] = prior[:, 128 * r - GROUP_COLS : 128 * r + GROUP_COLS]
    series[pl.ds(TICK_FIRST + TICK_ROWS, 8), :] = jnp.zeros((8, 128), jnp.float32)
    load.wait()

    lows = lax.broadcasted_iota(jnp.int32, (4, 128), 1) < GROUP_COLS

    def shifted(t, carry):
        row = FIRST_ROW + BLOCK_BARS * t
        for j in range(PIECES):
            here, after = series[pl.ds(row + 4 * j, 4), :], series[pl.ds(row + 4 * j + 1, 4), :]
            messages[t, j] = pltpu.roll(jnp.where(lows, after, here), GROUP_COLS, 1)
        return carry

    def aligned(t, carry):
        row = FIRST_ROW + BLOCK_BARS * t + 8
        for j in range(PIECES):
            messages[32 + t, j] = series[pl.ds(row + 4 * j, 4), :]
        return carry

    def assemble(target_half):
        @pl.when(target_half == 0)
        def _():
            lax.fori_loop(0, 32, shifted, 0, unroll=4)

        @pl.when(target_half == 1)
        def _():
            lax.fori_loop(0, 32, aligned, 0, unroll=4)

    assemble(half)
    pl.semaphore_wait(barrier, 33 + jnp.where(core == half, 0, 1))
    pl.semaphore_signal(far_ready, inc=1, device_id=(me, 1 - half), device_id_type=MESH)

    my_slot = half * 32 + pair

    def message(k):
        target_pair = lax.bitwise_xor(pair, lax.rem(k, 32))
        target_half = lax.bitwise_xor(half, k // 32)
        return target_pair, target_half, messages.at[target_half * 32 + target_pair]

    def remote(k):
        target_pair, target_half, src = message(k)
        return pltpu.make_async_remote_copy(
            src_ref=src,
            dst_ref=own_raw.at[my_slot],
            send_sem=send_sem,
            recv_sem=own_sem.at[my_slot // 8],
            device_id=(target_pair * 2 + core, target_half),
            device_id_type=MESH,
        )

    def send(k, carry):
        remote(k).start()
        return carry

    lax.fori_loop(1, 32, send, 0)
    _, _, kept = message(0)
    pltpu.make_async_copy(kept, own_raw.at[my_slot], own_sem.at[my_slot // 8]).start()

    assemble(1 - half)
    own_cols[...] = jnp.zeros_like(own_cols)
    other_cols[...] = jnp.zeros_like(other_cols)

    def clear(i, carry):
        at = pl.ds(pl.multiple_of(i * 256, 256), 256)
        for w in range(WIN_DEV):
            rows[w, at, :] = jnp.zeros((256, 128), jnp.float32)
            for first, last in ((0, 32 * w), (32 * w + 32, 128)):
                if last > first:
                    own[w, pl.ds(first, last - first), at] = jnp.zeros((last - first, 256), jnp.bfloat16)
                    other[w, pl.ds(first, last - first), at] = jnp.zeros((last - first, 256), jnp.bfloat16)
        return carry

    lax.fori_loop(0, TILE // 256, clear, 0)

    def chunk_of(q):
        return lax.bitwise_xor(my_slot // 8, q)

    def passing(q, w):
        at = pl.ds(pl.multiple_of(chunk_of(q) * 512, 512), 512)
        return pltpu.make_async_remote_copy(
            src_ref=own.at[w, pl.ds(32 * w, 32), at],
            dst_ref=other.at[w, pl.ds(32 * w, 32), at],
            send_sem=pass_sem.at[q, w],
            recv_sem=other_sem.at[q, w],
            device_id=(sibling, half),
            device_id_type=MESH,
        )

    def pass_on(q):
        for w in range(WIN_DEV):
            passing(q, w).start()

    def receive(q):
        ref = own_raw.at[pl.ds(chunk_of(q) * 8, 8)]
        pltpu.make_async_copy(ref, ref, own_sem.at[chunk_of(q)]).wait()

    def prepare_chunk(q):
        prepare(own_raw, bars, ready, turned, chunk_of(q))

    def settle_chunk(q):
        settle(ready, turned, own, lhs_ref, chunk_of(q))

    def block(i):
        return pl.ds(pl.multiple_of(i * BLOCK, BLOCK), BLOCK)

    def pairs(w, row_at, col_at, right, cols):
        a = magnitudes(lhs_ref[row_at, :], right[w, :, col_at])
        if cols is not None:
            cols[w, :, col_at] += fold_rows(a)
        return a[:, :128] + a[:, 128:]

    near, far = half * 8, 8 - half * 8

    def against(row_block, col_chunk, w):
        row_at = block(row_block)
        rows[w, row_at, :] += pairs(w, row_at, block(2 * col_chunk), own, own_cols) + pairs(
            w, row_at, block(2 * col_chunk + 1), own, own_cols
        )

    def with_chunk(q, r):
        for i in range(2):
            for w in range(WIN_DEV):
                against(2 * chunk_of(r) + i, chunk_of(q), w)

    def with_itself(q):
        first, second = block(2 * chunk_of(q)), block(2 * chunk_of(q) + 1)
        for w in range(WIN_DEV):
            rows[w, first, :] += pairs(w, first, first, own, None) + pairs(w, first, second, own, own_cols)
            rows[w, second, :] += pairs(w, second, second, own, None)

    def next_chunk(q):
        receive(q)
        prepare_chunk(q)

    next_chunk(0)
    pl.semaphore_wait(far_ready, 1)
    lax.fori_loop(32, GROUPS, send, 0, unroll=4)
    settle_chunk(0)
    with_itself(0)
    pass_on(0)
    for q in range(1, 4):
        next_chunk(q)
        settle_chunk(q)
        for r in range(q):
            with_chunk(q, r)
        with_itself(q)
        pass_on(q)

    def with_near(q, w, i):
        row_at = block(2 * chunk_of(q) + i)
        total = rows[w, row_at, :]
        for d in range(8):
            total = total + pairs(w, row_at, block(near + d), own, own_cols)
        rows[w, row_at, :] = total

    def late(q, carry):
        settle_chunk(q)
        for w in range(WIN_DEV):
            with_near(q, w, 0)
        pass_on(q)
        next_chunk(q + 1)
        for w in range(WIN_DEV):
            with_near(q, w, 1)
        return carry

    next_chunk(4)
    lax.fori_loop(4, 7, late, 0)
    settle_chunk(7)
    pass_on(7)
    for i in range(2):
        for w in range(WIN_DEV):
            with_near(7, w, i)

    def square(h, carry):
        for i in range(4):
            row_at = block(far + 4 * h + i)
            half_at = pl.ds(pl.multiple_of((far + i) * BLOCK + h * 128, 128), 128)
            for w in range(WIN_DEV):
                total = rows[w, row_at, :]
                for d in range(4):
                    col = far + lax.rem(4 * h + i + d, 8)
                    total = total + pairs(w, row_at, block(col), own, own_cols if d else None)
                rows[w, row_at, :] = total
                rows[w, half_at, :] += pairs(w, half_at, block(far + i + 4), own, own_cols)
        return carry

    lax.fori_loop(0, 2, square, 0)

    def finish_pass(q, carry):
        for w in range(WIN_DEV):
            passing(q, w).wait_send()
        return carry

    def receive_other(q, carry):
        for w in range(WIN_DEV):
            passing(q, w).wait_recv()
        return carry

    lax.fori_loop(0, 8, receive_other, 0)

    scale = math.sqrt(SPAN) / ASSETS

    def gather_sums(first_block, sums):
        at = pl.ds(pl.multiple_of(first_block * BLOCK, BLOCK), HALF)
        for w in range(WIN_DEV):
            one = pl.ds(w, 1)
            sums[core, one, :] = (line[one, at] + jnp.sum(own_cols[w, :, at], axis=0, keepdims=True)) * scale
            sums[1 - core, one, :] = jnp.sum(other_cols[w, :, at], axis=0, keepdims=True) * scale

    far_copy = pltpu.make_async_remote_copy(
        src_ref=far_sums,
        dst_ref=arrived.at[core],
        send_sem=result_send.at[0],
        recv_sem=result_recv.at[core],
        device_id=(pair * 2 + half, 1 - half),
        device_id_type=MESH,
    )
    near_copy = pltpu.make_async_remote_copy(
        src_ref=near_sums,
        dst_ref=arrived.at[core],
        send_sem=result_send.at[1],
        recv_sem=result_recv.at[core],
        device_id=(sibling, half),
        device_id_type=MESH,
    )

    def across(part, carry):
        row_first = jnp.where(lax.rem(part, 2) == 0, far, near)
        col_first = jnp.where(part < 2, far, near)
        for t in range(2):
            cols_from = col_first + 4 * lax.rem(t + core, 2)
            for i in range(4):
                at_block = row_first + 4 * t + i
                row_at = block(at_block)
                for w in range(WIN_DEV):
                    total = rows[w, row_at, :]
                    for d in range(4):
                        total = total + pairs(w, row_at, block(cols_from + d), other, other_cols)
                    rows[w, row_at, :] = total
                    for p in range(0, BLOCK, 128):
                        at = pl.ds(pl.multiple_of(at_block * BLOCK + p, 128), 128)
                        line[pl.ds(w, 1), at] = jnp.sum(total[p : p + 128].T, axis=0, keepdims=True)

        @pl.when(part == 2)
        def _():
            gather_sums(far, far_sums)

            sent = own_raw.at[pl.ds(0, GROUPS - 1)]
            pltpu.make_async_copy(sent, sent, send_sem).wait()
            lax.fori_loop(0, 8, finish_pass, 0)
            far_copy.start()

        return carry

    lax.fori_loop(0, 4, across, 0)
    gather_sums(near, near_sums)

    lanes_low = lax.broadcasted_iota(jnp.int32, (WIN_DEV, 128), 1) < GROUP_COLS

    def write_out(first, second):
        for p in range(HALF // 128):
            at = pl.ds(p * 128, 128)
            zero = first[0, :, at] + second[0, :, at]
            one = first[1, :, at] + second[1, :, at]
            out_ref[:, pl.ds(2 * p * 128, 128)] = jnp.where(lanes_low, zero, pltpu.roll(one, GROUP_COLS, 1))
            out_ref[:, pl.ds((2 * p + 1) * 128, 128)] = jnp.where(lanes_low, pltpu.roll(zero, GROUP_COLS, 1), one)

    @pl.when(core != half)
    def _():
        near_copy.start()
        for d in range(2):
            pltpu.make_async_copy(arrived.at[d], arrived.at[d], result_recv.at[d]).wait()
        write_out(arrived.at[0], arrived.at[1])
        near_copy.wait_send()

    @pl.when(core == half)
    def _():
        other_core = 1 - core
        pltpu.make_async_copy(arrived.at[other_core], arrived.at[other_core], result_recv.at[other_core]).wait()
        write_out(near_sums, arrived.at[other_core])

    far_copy.wait_send()


def shards(tick_bars, prior_bars):
    return pl.pallas_call(
        kernel,
        out_shape=jax.ShapeDtypeStruct((WIN_DEV, TILE), jnp.float32),
        in_specs=[pl.BlockSpec(memory_space=pl.ANY)] * 2,
        out_specs=pl.BlockSpec(memory_space=pltpu.VMEM),
        scratch_shapes=[
            pltpu.VMEM((SERIES_ROWS, 128), jnp.float32),
            pltpu.VMEM((1, LEAD * GROUP_COLS), jnp.float32),
            pltpu.VMEM((GROUPS, PIECES, 4, 128), jnp.float32),
            pltpu.VMEM((GROUPS, PIECES, 4, 128), jnp.float32),
            pltpu.VMEM((2, 4, 24, 128), jnp.float32),
            pltpu.VMEM((WIN_DEV, 32, 512), jnp.bfloat16),
            pltpu.VMEM((512, 128), jnp.bfloat16),
            pltpu.VMEM((WIN_DEV, 128, TILE), jnp.bfloat16),
            pltpu.VMEM((WIN_DEV, 128, TILE), jnp.bfloat16),
            pltpu.VMEM((TILE, 128), jnp.bfloat16),
            pltpu.VMEM((WIN_DEV, TILE, 128), jnp.float32),
            pltpu.VMEM((WIN_DEV, 8, TILE), jnp.float32),
            pltpu.VMEM((WIN_DEV, 8, TILE), jnp.float32),
            pltpu.VMEM((WIN_DEV, TILE), jnp.float32),
            pltpu.VMEM((2, WIN_DEV, HALF), jnp.float32),
            pltpu.VMEM((2, WIN_DEV, HALF), jnp.float32),
            pltpu.VMEM((2, 2, WIN_DEV, HALF), jnp.float32),
            pltpu.SemaphoreType.DMA((2,)),
            pltpu.SemaphoreType.DMA,
            pltpu.SemaphoreType.DMA((8,)),
            pltpu.SemaphoreType.DMA((8, WIN_DEV)),
            pltpu.SemaphoreType.DMA((8, WIN_DEV)),
            pltpu.SemaphoreType.DMA((2,)),
            pltpu.SemaphoreType.DMA((2,)),
            pltpu.SemaphoreType.REGULAR,
        ],
        compiler_params=pltpu.CompilerParams(collective_id=0, has_side_effects=True, vmem_limit_bytes=56 * 2**20),
        name="connect",
    )(tick_bars.reshape(TICK_ROWS, 128), prior_bars.reshape(1, LEAD * GROUP_COLS))


def solution(mesh):
    in_specs = (P("asset", "tm", None), P("asset", "tm", None))
    out_specs = P("tm", "asset")
    return jax.shard_map(shards, mesh=mesh, in_specs=in_specs, out_specs=out_specs, check_vma=False)
```

```python
import functools
import math

import jax
import jax.numpy as jnp
from jax import lax
from jax.experimental import pallas as pl
from jax.experimental.pallas import tpu as pltpu
from jax.sharding import PartitionSpec as P

ASSETS = 8192
SPAN = 30
STRIDE = 5
WIN_DEV = 3
LEAD = 25
FLOOR_SQUARES = 1.0

MESH = pl.DeviceIdType.MESH
TILE = ASSETS // 2
GROUPS = 64
GROUP_COLS = TILE // GROUPS
BLOCK_BARS = WIN_DEV * STRIDE
FIRST_ROW = 3
TICK_FIRST = 16
TICK_ROWS = 480
SERIES_ROWS = TICK_FIRST + TICK_ROWS + 8
PIECES = 5
BLOCK = 256
HALF = TILE // 2


def place():
    tm = lax.axis_index("tm")
    return tm // 2, lax.rem(tm, 2), lax.axis_index("asset")


def magnitudes(lhs, rhs):
    return jnp.abs(
        lax.dot_general(lhs, rhs, (((1,), (0,)), ((), ())), preferred_element_type=jnp.float32)
    )


def fold_rows(a):
    return jnp.sum(a.reshape(a.shape[0] // 8, 8, a.shape[1]), axis=0)


def prepare(raw_ref, bars, ready, turned, chunk):
    low = lax.broadcasted_iota(jnp.int32, (4, 128), 1) < GROUP_COLS
    valid = lax.broadcasted_iota(jnp.int32, (16, 128), 0) < SPAN // 2
    for p in range(4):
        slot = chunk * 8 + 2 * p
        for j in range(PIECES):
            a, b = raw_ref[slot, j], raw_ref[slot + 1, j]
            bars[0, p, pl.ds(4 * j, 4), :] = jnp.where(low, a, pltpu.roll(b, GROUP_COLS, 1))
            bars[1, p, pl.ds(4 * j, 4), :] = jnp.where(low, pltpu.roll(a, GROUP_COLS, 1), b)
    for p in range(4):
        at = pl.ds(p * 128, 128)
        parts = []
        for w in range(WIN_DEV):
            first = w * STRIDE
            even = jnp.where(valid, bars[0, p, pl.ds((first + 1) // 2, 16), :], 0.0)
            odd = jnp.where(valid, bars[1, p, pl.ds(first // 2, 16), :], 0.0)
            mean = jnp.sum(even + odd, axis=0, keepdims=True) * (1.0 / SPAN)
            even = jnp.where(valid, even - mean, 0.0)
            odd = jnp.where(valid, odd - mean, 0.0)
            squares = jnp.sum(even * even + odd * odd, axis=0, keepdims=True)
            scale = lax.rsqrt(jnp.maximum(squares, FLOOR_SQUARES))
            even, odd = (even * scale).astype(jnp.bfloat16), (odd * scale).astype(jnp.bfloat16)
            ready[w, pl.ds(0, 16), at] = even
            ready[w, pl.ds(16, 16), at] = odd
            parts += [even, odd]
        parts.append(jnp.zeros((32, 128), jnp.bfloat16))
        turned[at, :] = jnp.concatenate(parts, axis=0).T


def settle(ready, turned, scaled, lhs_ref, chunk):
    at = pl.ds(pl.multiple_of(chunk * 512, 512), 512)
    for w in range(WIN_DEV):
        scaled[w, pl.ds(32 * w, 32), at] = ready[w]
    lhs_ref[at, :] = turned[...]


def kernel(
    tick_ref, prior_ref, out_ref, series, prior, messages, own_raw, bars, ready, turned, own, other, lhs_ref, rows, own_cols, other_cols, line, far_sums, near_sums, arrived,
    load_sem, send_sem, own_sem, pass_sem, other_sem, result_send, result_recv, far_ready,
):
    pair, core, half = place()
    me = pair * 2 + core
    sibling = pair * 2 + 1 - core
    prior_load = pltpu.make_async_copy(prior_ref, prior, load_sem.at[0])
    prior_load.start()
    load = pltpu.make_async_copy(tick_ref, series.at[pl.ds(TICK_FIRST, TICK_ROWS)], load_sem.at[1])
    load.start()

    barrier = pltpu.get_barrier_semaphore()

    def greet(j, carry):
        target = 2 * lax.bitwise_xor(pair, 31 - j) + core
        pl.semaphore_signal(barrier, inc=1, device_id=(target, half), device_id_type=MESH)
        return carry

    lax.fori_loop(0, 31, greet, 0)
    pl.semaphore_signal(barrier, inc=1, device_id=(sibling, half), device_id_type=MESH)
    pl.semaphore_signal(barrier, inc=1, device_id=(me, 1 - half), device_id_type=MESH)

    @pl.when(core != half)
    def _():
        pl.semaphore_signal(barrier, inc=1, device_id=(sibling, core), device_id_type=MESH)

    prior_load.wait()
    low = lax.broadcasted_iota(jnp.int32, (1, 128), 1) < GROUP_COLS
    series[pl.ds(FIRST_ROW, 1), :] = jnp.where(low, 0.0, pltpu.roll(prior[:, 0:128], GROUP_COLS, 1))
    for r in range(1, TICK_FIRST - FIRST_ROW):
        series[pl.ds(FIRST_ROW + r, 1), :] = prior[:, 128 * r - GROUP_COLS : 128 * r + GROUP_COLS]
    series[pl.ds(TICK_FIRST + TICK_ROWS, 8), :] = jnp.zeros((8, 128), jnp.float32)
    load.wait()

    lows = lax.broadcasted_iota(jnp.int32, (4, 128), 1) < GROUP_COLS

    def shifted(t, carry):
        row = FIRST_ROW + BLOCK_BARS * t
        for j in range(PIECES):
            here, after = series[pl.ds(row + 4 * j, 4), :], series[pl.ds(row + 4 * j + 1, 4), :]
            messages[t, j] = pltpu.roll(jnp.where(lows, after, here), GROUP_COLS, 1)
        return carry

    def aligned(t, carry):
        row = FIRST_ROW + BLOCK_BARS * t + 8
        for j in range(PIECES):
            messages[32 + t, j] = series[pl.ds(row + 4 * j, 4), :]
        return carry

    def assemble(target_half):
        @pl.when(target_half == 0)
        def _():
            lax.fori_loop(0, 32, shifted, 0, unroll=4)

        @pl.when(target_half == 1)
        def _():
            lax.fori_loop(0, 32, aligned, 0, unroll=4)

    assemble(half)
    pl.semaphore_wait(barrier, 33 + jnp.where(core == half, 0, 1))
    pl.semaphore_signal(far_ready, inc=1, device_id=(me, 1 - half), device_id_type=MESH)

    my_slot = half * 32 + pair

    def message(k):
        target_pair = lax.bitwise_xor(pair, lax.rem(k, 32))
        target_half = lax.bitwise_xor(half, k // 32)
        return target_pair, target_half, messages.at[target_half * 32 + target_pair]

    def remote(k):
        target_pair, target_half, src = message(k)
        return pltpu.make_async_remote_copy(
            src_ref=src,
            dst_ref=own_raw.at[my_slot],
            send_sem=send_sem,
            recv_sem=own_sem.at[my_slot // 8],
            device_id=(target_pair * 2 + core, target_half),
            device_id_type=MESH,
        )

    def send(k, carry):
        remote(k).start()
        return carry

    lax.fori_loop(1, 32, send, 0)
    _, _, kept = message(0)
    pltpu.make_async_copy(kept, own_raw.at[my_slot], own_sem.at[my_slot // 8]).start()

    assemble(1 - half)
    own_cols[...] = jnp.zeros_like(own_cols)
    other_cols[...] = jnp.zeros_like(other_cols)

    def clear(i, carry):
        at = pl.ds(pl.multiple_of(i * 256, 256), 256)
        for w in range(WIN_DEV):
            rows[w, at, :] = jnp.zeros((256, 128), jnp.float32)
            for first, last in ((0, 32 * w), (32 * w + 32, 128)):
                if last > first:
                    own[w, pl.ds(first, last - first), at] = jnp.zeros((last - first, 256), jnp.bfloat16)
                    other[w, pl.ds(first, last - first), at] = jnp.zeros((last - first, 256), jnp.bfloat16)
        return carry

    lax.fori_loop(0, TILE // 256, clear, 0)

    def chunk_of(q):
        return lax.bitwise_xor(my_slot // 8, q)

    def passing(q, w):
        at = pl.ds(pl.multiple_of(chunk_of(q) * 512, 512), 512)
        return pltpu.make_async_remote_copy(
            src_ref=own.at[w, pl.ds(32 * w, 32), at],
            dst_ref=other.at[w, pl.ds(32 * w, 32), at],
            send_sem=pass_sem.at[q, w],
            recv_sem=other_sem.at[q, w],
            device_id=(sibling, half),
            device_id_type=MESH,
        )

    def pass_on(q):
        for w in range(WIN_DEV):
            passing(q, w).start()

    def receive(q):
        ref = own_raw.at[pl.ds(chunk_of(q) * 8, 8)]
        pltpu.make_async_copy(ref, ref, own_sem.at[chunk_of(q)]).wait()

    def prepare_chunk(q):
        prepare(own_raw, bars, ready, turned, chunk_of(q))

    def settle_chunk(q):
        settle(ready, turned, own, lhs_ref, chunk_of(q))

    def block(i):
        return pl.ds(pl.multiple_of(i * BLOCK, BLOCK), BLOCK)

    def pairs(w, row_at, col_at, right, cols):
        a = magnitudes(lhs_ref[row_at, :], right[w, :, col_at])
        if cols is not None:
            cols[w, :, col_at] += fold_rows(a)
        return a[:, :128] + a[:, 128:]

    near, far = half * 8, 8 - half * 8

    def against(row_block, col_chunk, w):
        row_at = block(row_block)
        rows[w, row_at, :] += pairs(w, row_at, block(2 * col_chunk), own, own_cols) + pairs(
            w, row_at, block(2 * col_chunk + 1), own, own_cols
        )

    def with_chunk(q, r):
        for i in range(2):
            for w in range(WIN_DEV):
                against(2 * chunk_of(r) + i, chunk_of(q), w)

    def with_itself(q):
        first, second = block(2 * chunk_of(q)), block(2 * chunk_of(q) + 1)
        for w in range(WIN_DEV):
            rows[w, first, :] += pairs(w, first, first, own, None) + pairs(w, first, second, own, own_cols)
            rows[w, second, :] += pairs(w, second, second, own, None)

    def next_chunk(q):
        receive(q)
        prepare_chunk(q)

    receive(0)
    pl.semaphore_wait(far_ready, 1)
    lax.fori_loop(32, 48, send, 0, unroll=4)
    prepare_chunk(0)
    settle_chunk(0)
    with_itself(0)
    pass_on(0)
    for q in range(1, 4):
        receive(q)
        if q == 1:
            lax.fori_loop(48, GROUPS, send, 0, unroll=4)
        prepare_chunk(q)
        settle_chunk(q)
        for r in range(q):
            with_chunk(q, r)
        with_itself(q)
        pass_on(q)

    def with_near(q, w, i):
        row_at = block(2 * chunk_of(q) + i)
        total = rows[w, row_at, :]
        for d in range(8):
            total = total + pairs(w, row_at, block(near + d), own, own_cols)
        rows[w, row_at, :] = total

    def late(q, carry):
        settle_chunk(q)
        for w in range(WIN_DEV):
            with_near(q, w, 0)
        pass_on(q)
        next_chunk(q + 1)
        for w in range(WIN_DEV):
            with_near(q, w, 1)
        return carry

    next_chunk(4)
    lax.fori_loop(4, 7, late, 0)
    settle_chunk(7)
    pass_on(7)
    for i in range(2):
        for w in range(WIN_DEV):
            with_near(7, w, i)

    def square(h, carry):
        for i in range(4):
            row_at = block(far + 4 * h + i)
            half_at = pl.ds(pl.multiple_of((far + i) * BLOCK + h * 128, 128), 128)
            for w in range(WIN_DEV):
                total = rows[w, row_at, :]
                for d in range(4):
                    col = far + lax.rem(4 * h + i + d, 8)
                    total = total + pairs(w, row_at, block(col), own, own_cols if d else None)
                rows[w, row_at, :] = total
                rows[w, half_at, :] += pairs(w, half_at, block(far + i + 4), own, own_cols)
        return carry

    lax.fori_loop(0, 2, square, 0)

    def finish_pass(q, carry):
        for w in range(WIN_DEV):
            passing(q, w).wait_send()
        return carry

    def receive_other(q, carry):
        for w in range(WIN_DEV):
            passing(q, w).wait_recv()
        return carry

    lax.fori_loop(0, 8, receive_other, 0)

    scale = math.sqrt(SPAN) / ASSETS

    def gather_sums(first_block, sums):
        at = pl.ds(pl.multiple_of(first_block * BLOCK, BLOCK), HALF)
        for w in range(WIN_DEV):
            one = pl.ds(w, 1)
            sums[core, one, :] = (line[one, at] + jnp.sum(own_cols[w, :, at], axis=0, keepdims=True)) * scale
            sums[1 - core, one, :] = jnp.sum(other_cols[w, :, at], axis=0, keepdims=True) * scale

    far_copy = pltpu.make_async_remote_copy(
        src_ref=far_sums,
        dst_ref=arrived.at[core],
        send_sem=result_send.at[0],
        recv_sem=result_recv.at[core],
        device_id=(pair * 2 + half, 1 - half),
        device_id_type=MESH,
    )
    near_copy = pltpu.make_async_remote_copy(
        src_ref=near_sums,
        dst_ref=arrived.at[core],
        send_sem=result_send.at[1],
        recv_sem=result_recv.at[core],
        device_id=(sibling, half),
        device_id_type=MESH,
    )

    def across(part, carry):
        row_first = jnp.where(lax.rem(part, 2) == 0, far, near)
        col_first = jnp.where(part < 2, far, near)
        for t in range(2):
            cols_from = col_first + 4 * lax.rem(t + core, 2)
            for i in range(4):
                at_block = row_first + 4 * t + i
                row_at = block(at_block)
                for w in range(WIN_DEV):
                    total = rows[w, row_at, :]
                    for d in range(4):
                        total = total + pairs(w, row_at, block(cols_from + d), other, other_cols)
                    rows[w, row_at, :] = total
                    for p in range(0, BLOCK, 128):
                        at = pl.ds(pl.multiple_of(at_block * BLOCK + p, 128), 128)
                        line[pl.ds(w, 1), at] = jnp.sum(total[p : p + 128].T, axis=0, keepdims=True)

        @pl.when(part == 2)
        def _():
            gather_sums(far, far_sums)

            sent = own_raw.at[pl.ds(0, GROUPS - 1)]
            pltpu.make_async_copy(sent, sent, send_sem).wait()
            lax.fori_loop(0, 8, finish_pass, 0)
            far_copy.start()

        return carry

    lax.fori_loop(0, 4, across, 0)
    gather_sums(near, near_sums)

    lanes_low = lax.broadcasted_iota(jnp.int32, (WIN_DEV, 128), 1) < GROUP_COLS

    def write_out(first, second):
        for p in range(HALF // 128):
            at = pl.ds(p * 128, 128)
            zero = first[0, :, at] + second[0, :, at]
            one = first[1, :, at] + second[1, :, at]
            out_ref[:, pl.ds(2 * p * 128, 128)] = jnp.where(lanes_low, zero, pltpu.roll(one, GROUP_COLS, 1))
            out_ref[:, pl.ds((2 * p + 1) * 128, 128)] = jnp.where(lanes_low, pltpu.roll(zero, GROUP_COLS, 1), one)

    @pl.when(core != half)
    def _():
        near_copy.start()
        for d in range(2):
            pltpu.make_async_copy(arrived.at[d], arrived.at[d], result_recv.at[d]).wait()
        write_out(arrived.at[0], arrived.at[1])
        near_copy.wait_send()

    @pl.when(core == half)
    def _():
        other_core = 1 - core
        pltpu.make_async_copy(arrived.at[other_core], arrived.at[other_core], result_recv.at[other_core]).wait()
        write_out(near_sums, arrived.at[other_core])

    far_copy.wait_send()


def shards(tick_bars, prior_bars):
    return pl.pallas_call(
        kernel,
        out_shape=jax.ShapeDtypeStruct((WIN_DEV, TILE), jnp.float32),
        in_specs=[pl.BlockSpec(memory_space=pl.ANY)] * 2,
        out_specs=pl.BlockSpec(memory_space=pltpu.VMEM),
        scratch_shapes=[
            pltpu.VMEM((SERIES_ROWS, 128), jnp.float32),
            pltpu.VMEM((1, LEAD * GROUP_COLS), jnp.float32),
            pltpu.VMEM((GROUPS, PIECES, 4, 128), jnp.float32),
            pltpu.VMEM((GROUPS, PIECES, 4, 128), jnp.float32),
            pltpu.VMEM((2, 4, 24, 128), jnp.float32),
            pltpu.VMEM((WIN_DEV, 32, 512), jnp.bfloat16),
            pltpu.VMEM((512, 128), jnp.bfloat16),
            pltpu.VMEM((WIN_DEV, 128, TILE), jnp.bfloat16),
            pltpu.VMEM((WIN_DEV, 128, TILE), jnp.bfloat16),
            pltpu.VMEM((TILE, 128), jnp.bfloat16),
            pltpu.VMEM((WIN_DEV, TILE, 128), jnp.float32),
            pltpu.VMEM((WIN_DEV, 8, TILE), jnp.float32),
            pltpu.VMEM((WIN_DEV, 8, TILE), jnp.float32),
            pltpu.VMEM((WIN_DEV, TILE), jnp.float32),
            pltpu.VMEM((2, WIN_DEV, HALF), jnp.float32),
            pltpu.VMEM((2, WIN_DEV, HALF), jnp.float32),
            pltpu.VMEM((2, 2, WIN_DEV, HALF), jnp.float32),
            pltpu.SemaphoreType.DMA((2,)),
            pltpu.SemaphoreType.DMA,
            pltpu.SemaphoreType.DMA((8,)),
            pltpu.SemaphoreType.DMA((8, WIN_DEV)),
            pltpu.SemaphoreType.DMA((8, WIN_DEV)),
            pltpu.SemaphoreType.DMA((2,)),
            pltpu.SemaphoreType.DMA((2,)),
            pltpu.SemaphoreType.REGULAR,
        ],
        compiler_params=pltpu.CompilerParams(collective_id=0, has_side_effects=True, vmem_limit_bytes=56 * 2**20),
        name="connect",
    )(tick_bars.reshape(TICK_ROWS, 128), prior_bars.reshape(1, LEAD * GROUP_COLS))


def solution(mesh):
    in_specs = (P("asset", "tm", None), P("asset", "tm", None))
    out_specs = P("tm", "asset")
    return jax.shard_map(shards, mesh=mesh, in_specs=in_specs, out_specs=out_specs, check_vma=False)
```

```python
import functools
import math

import jax
import jax.numpy as jnp
from jax import lax
from jax.experimental import pallas as pl
from jax.experimental.pallas import tpu as pltpu
from jax.sharding import PartitionSpec as P

ASSETS = 8192
SPAN = 30
STRIDE = 5
WIN_DEV = 3
LEAD = 25
FLOOR_SQUARES = 1.0

MESH = pl.DeviceIdType.MESH
TILE = ASSETS // 2
GROUPS = 64
GROUP_COLS = TILE // GROUPS
BLOCK_BARS = WIN_DEV * STRIDE
FIRST_ROW = 3
TICK_FIRST = 16
TICK_ROWS = 480
SERIES_ROWS = TICK_FIRST + TICK_ROWS + 8
PIECES = 5
BLOCK = 256
HALF = TILE // 2


def place():
    tm = lax.axis_index("tm")
    return tm // 2, lax.rem(tm, 2), lax.axis_index("asset")


def magnitudes(lhs, rhs):
    return jnp.abs(
        lax.dot_general(lhs, rhs, (((1,), (0,)), ((), ())), preferred_element_type=jnp.float32)
    )


def fold_rows(a):
    return jnp.sum(a.reshape(a.shape[0] // 8, 8, a.shape[1]), axis=0)


def prepare(raw_ref, bars, ready, turned, chunk):
    low = lax.broadcasted_iota(jnp.int32, (4, 128), 1) < GROUP_COLS
    valid = lax.broadcasted_iota(jnp.int32, (16, 128), 0) < SPAN // 2
    for p in range(4):
        slot = chunk * 8 + 2 * p
        for j in range(PIECES):
            a, b = raw_ref[slot, j], raw_ref[slot + 1, j]
            bars[0, p, pl.ds(4 * j, 4), :] = jnp.where(low, a, pltpu.roll(b, GROUP_COLS, 1))
            bars[1, p, pl.ds(4 * j, 4), :] = jnp.where(low, pltpu.roll(a, GROUP_COLS, 1), b)
    for p in range(4):
        at = pl.ds(p * 128, 128)
        parts = []
        for w in range(WIN_DEV):
            first = w * STRIDE
            even = jnp.where(valid, bars[0, p, pl.ds((first + 1) // 2, 16), :], 0.0)
            odd = jnp.where(valid, bars[1, p, pl.ds(first // 2, 16), :], 0.0)
            mean = jnp.sum(even + odd, axis=0, keepdims=True) * (1.0 / SPAN)
            even = jnp.where(valid, even - mean, 0.0)
            odd = jnp.where(valid, odd - mean, 0.0)
            squares = jnp.sum(even * even + odd * odd, axis=0, keepdims=True)
            scale = lax.rsqrt(jnp.maximum(squares, FLOOR_SQUARES))
            even, odd = (even * scale).astype(jnp.bfloat16), (odd * scale).astype(jnp.bfloat16)
            ready[w, pl.ds(0, 16), at] = even
            ready[w, pl.ds(16, 16), at] = odd
            parts += [even, odd]
        parts.append(jnp.zeros((32, 128), jnp.bfloat16))
        turned[at, :] = jnp.concatenate(parts, axis=0).T


def settle(ready, turned, scaled, lhs_ref, chunk):
    at = pl.ds(pl.multiple_of(chunk * 512, 512), 512)
    for w in range(WIN_DEV):
        scaled[w, pl.ds(32 * w, 32), at] = ready[w]
    lhs_ref[at, :] = turned[...]


def kernel(
    tick_ref, prior_ref, out_ref, series, prior, messages, own_raw, bars, ready, turned, own, other, lhs_ref, rows, own_cols, other_cols, line, far_sums, near_sums, arrived,
    load_sem, send_sem, own_sem, pass_sem, other_sem, result_send, result_recv, far_ready,
):
    pair, core, half = place()
    me = pair * 2 + core
    sibling = pair * 2 + 1 - core
    prior_load = pltpu.make_async_copy(prior_ref, prior, load_sem.at[0])
    prior_load.start()
    load = pltpu.make_async_copy(tick_ref, series.at[pl.ds(TICK_FIRST, TICK_ROWS)], load_sem.at[1])
    load.start()

    barrier = pltpu.get_barrier_semaphore()

    def greet(j, carry):
        target = 2 * lax.bitwise_xor(pair, 31 - j) + core
        pl.semaphore_signal(barrier, inc=1, device_id=(target, half), device_id_type=MESH)
        return carry

    lax.fori_loop(0, 31, greet, 0, unroll=4)
    pl.semaphore_signal(barrier, inc=1, device_id=(sibling, half), device_id_type=MESH)
    pl.semaphore_signal(barrier, inc=1, device_id=(me, 1 - half), device_id_type=MESH)

    @pl.when(core != half)
    def _():
        pl.semaphore_signal(barrier, inc=1, device_id=(sibling, core), device_id_type=MESH)

    prior_load.wait()
    low = lax.broadcasted_iota(jnp.int32, (1, 128), 1) < GROUP_COLS
    series[pl.ds(FIRST_ROW, 1), :] = jnp.where(low, 0.0, pltpu.roll(prior[:, 0:128], GROUP_COLS, 1))
    for r in range(1, TICK_FIRST - FIRST_ROW):
        series[pl.ds(FIRST_ROW + r, 1), :] = prior[:, 128 * r - GROUP_COLS : 128 * r + GROUP_COLS]
    series[pl.ds(TICK_FIRST + TICK_ROWS, 8), :] = jnp.zeros((8, 128), jnp.float32)
    load.wait()

    lows = lax.broadcasted_iota(jnp.int32, (4, 128), 1) < GROUP_COLS

    def shifted(t, carry):
        row = FIRST_ROW + BLOCK_BARS * t
        for j in range(PIECES):
            here, after = series[pl.ds(row + 4 * j, 4), :], series[pl.ds(row + 4 * j + 1, 4), :]
            messages[t, j] = pltpu.roll(jnp.where(lows, after, here), GROUP_COLS, 1)
        return carry

    def aligned(t, carry):
        row = FIRST_ROW + BLOCK_BARS * t + 8
        for j in range(PIECES):
            messages[32 + t, j] = series[pl.ds(row + 4 * j, 4), :]
        return carry

    def assemble(target_half):
        @pl.when(target_half == 0)
        def _():
            lax.fori_loop(0, 32, shifted, 0, unroll=4)

        @pl.when(target_half == 1)
        def _():
            lax.fori_loop(0, 32, aligned, 0, unroll=4)

    assemble(half)
    pl.semaphore_wait(barrier, 33 + jnp.where(core == half, 0, 1))
    pl.semaphore_signal(far_ready, inc=1, device_id=(me, 1 - half), device_id_type=MESH)

    my_slot = half * 32 + pair

    def message(k):
        target_pair = lax.bitwise_xor(pair, lax.rem(k, 32))
        target_half = lax.bitwise_xor(half, k // 32)
        return target_pair, target_half, messages.at[target_half * 32 + target_pair]

    def remote(k):
        target_pair, target_half, src = message(k)
        return pltpu.make_async_remote_copy(
            src_ref=src,
            dst_ref=own_raw.at[my_slot],
            send_sem=send_sem,
            recv_sem=own_sem.at[my_slot // 8],
            device_id=(target_pair * 2 + core, target_half),
            device_id_type=MESH,
        )

    def send(k, carry):
        remote(k).start()
        return carry

    lax.fori_loop(1, 32, send, 0, unroll=4)
    _, _, kept = message(0)
    pltpu.make_async_copy(kept, own_raw.at[my_slot], own_sem.at[my_slot // 8]).start()

    assemble(1 - half)
    own_cols[...] = jnp.zeros_like(own_cols)
    other_cols[...] = jnp.zeros_like(other_cols)

    def clear(i, carry):
        at = pl.ds(pl.multiple_of(i * 256, 256), 256)
        for w in range(WIN_DEV):
            rows[w, at, :] = jnp.zeros((256, 128), jnp.float32)
            for first, last in ((0, 32 * w), (32 * w + 32, 128)):
                if last > first:
                    own[w, pl.ds(first, last - first), at] = jnp.zeros((last - first, 256), jnp.bfloat16)
                    other[w, pl.ds(first, last - first), at] = jnp.zeros((last - first, 256), jnp.bfloat16)
        return carry

    lax.fori_loop(0, TILE // 256, clear, 0)

    def chunk_of(q):
        return lax.bitwise_xor(my_slot // 8, q)

    def passing(q, w):
        at = pl.ds(pl.multiple_of(chunk_of(q) * 512, 512), 512)
        return pltpu.make_async_remote_copy(
            src_ref=own.at[w, pl.ds(32 * w, 32), at],
            dst_ref=other.at[w, pl.ds(32 * w, 32), at],
            send_sem=pass_sem.at[q, w],
            recv_sem=other_sem.at[q, w],
            device_id=(sibling, half),
            device_id_type=MESH,
        )

    def pass_on(q):
        for w in range(WIN_DEV):
            passing(q, w).start()

    def receive(q):
        ref = own_raw.at[pl.ds(chunk_of(q) * 8, 8)]
        pltpu.make_async_copy(ref, ref, own_sem.at[chunk_of(q)]).wait()

    def prepare_chunk(q):
        prepare(own_raw, bars, ready, turned, chunk_of(q))

    def settle_chunk(q):
        settle(ready, turned, own, lhs_ref, chunk_of(q))

    def block(i):
        return pl.ds(pl.multiple_of(i * BLOCK, BLOCK), BLOCK)

    def pairs(w, row_at, col_at, right, cols):
        a = magnitudes(lhs_ref[row_at, :], right[w, :, col_at])
        if cols is not None:
            cols[w, :, col_at] += fold_rows(a)
        return a[:, :128] + a[:, 128:]

    near, far = half * 8, 8 - half * 8

    def against(row_block, col_chunk, w):
        row_at = block(row_block)
        rows[w, row_at, :] += pairs(w, row_at, block(2 * col_chunk), own, own_cols) + pairs(
            w, row_at, block(2 * col_chunk + 1), own, own_cols
        )

    def with_chunk(q, r):
        for i in range(2):
            for w in range(WIN_DEV):
                against(2 * chunk_of(r) + i, chunk_of(q), w)

    def with_itself(q):
        first, second = block(2 * chunk_of(q)), block(2 * chunk_of(q) + 1)
        for w in range(WIN_DEV):
            rows[w, first, :] += pairs(w, first, first, own, None) + pairs(w, first, second, own, own_cols)
            rows[w, second, :] += pairs(w, second, second, own, None)

    def next_chunk(q):
        receive(q)
        prepare_chunk(q)

    receive(0)
    pl.semaphore_wait(far_ready, 1)
    lax.fori_loop(32, 48, send, 0, unroll=4)
    prepare_chunk(0)
    settle_chunk(0)
    with_itself(0)
    pass_on(0)
    for q in range(1, 4):
        receive(q)
        if q == 1:
            lax.fori_loop(48, GROUPS, send, 0, unroll=4)
        prepare_chunk(q)
        settle_chunk(q)
        for r in range(q):
            with_chunk(q, r)
        with_itself(q)
        pass_on(q)

    def with_near(q, w, i):
        row_at = block(2 * chunk_of(q) + i)
        total = rows[w, row_at, :]
        for d in range(8):
            total = total + pairs(w, row_at, block(near + d), own, own_cols)
        rows[w, row_at, :] = total

    def late(q, carry):
        settle_chunk(q)
        for w in range(WIN_DEV):
            with_near(q, w, 0)
        pass_on(q)
        next_chunk(q + 1)
        for w in range(WIN_DEV):
            with_near(q, w, 1)
        return carry

    next_chunk(4)
    lax.fori_loop(4, 7, late, 0)
    settle_chunk(7)
    pass_on(7)
    for i in range(2):
        for w in range(WIN_DEV):
            with_near(7, w, i)

    def square(h, carry):
        for i in range(4):
            row_at = block(far + 4 * h + i)
            half_at = pl.ds(pl.multiple_of((far + i) * BLOCK + h * 128, 128), 128)
            for w in range(WIN_DEV):
                total = rows[w, row_at, :]
                for d in range(4):
                    col = far + lax.rem(4 * h + i + d, 8)
                    total = total + pairs(w, row_at, block(col), own, own_cols if d else None)
                rows[w, row_at, :] = total
                rows[w, half_at, :] += pairs(w, half_at, block(far + i + 4), own, own_cols)
        return carry

    lax.fori_loop(0, 2, square, 0)

    def finish_pass(q, carry):
        for w in range(WIN_DEV):
            passing(q, w).wait_send()
        return carry

    def receive_other(q, carry):
        for w in range(WIN_DEV):
            passing(q, w).wait_recv()
        return carry

    lax.fori_loop(0, 8, receive_other, 0)

    scale = math.sqrt(SPAN) / ASSETS

    def gather_sums(first_block, sums):
        at = pl.ds(pl.multiple_of(first_block * BLOCK, BLOCK), HALF)
        for w in range(WIN_DEV):
            one = pl.ds(w, 1)
            sums[core, one, :] = (line[one, at] + jnp.sum(own_cols[w, :, at], axis=0, keepdims=True)) * scale
            sums[1 - core, one, :] = jnp.sum(other_cols[w, :, at], axis=0, keepdims=True) * scale

    far_copy = pltpu.make_async_remote_copy(
        src_ref=far_sums,
        dst_ref=arrived.at[core],
        send_sem=result_send.at[0],
        recv_sem=result_recv.at[core],
        device_id=(pair * 2 + half, 1 - half),
        device_id_type=MESH,
    )
    near_copy = pltpu.make_async_remote_copy(
        src_ref=near_sums,
        dst_ref=arrived.at[core],
        send_sem=result_send.at[1],
        recv_sem=result_recv.at[core],
        device_id=(sibling, half),
        device_id_type=MESH,
    )

    def across(part, carry):
        row_first = jnp.where(lax.rem(part, 2) == 0, far, near)
        col_first = jnp.where(part < 2, far, near)
        for t in range(2):
            cols_from = col_first + 4 * lax.rem(t + core, 2)
            for i in range(4):
                at_block = row_first + 4 * t + i
                row_at = block(at_block)
                for w in range(WIN_DEV):
                    total = rows[w, row_at, :]
                    for d in range(4):
                        total = total + pairs(w, row_at, block(cols_from + d), other, other_cols)
                    rows[w, row_at, :] = total
                    for p in range(0, BLOCK, 128):
                        at = pl.ds(pl.multiple_of(at_block * BLOCK + p, 128), 128)
                        line[pl.ds(w, 1), at] = jnp.sum(total[p : p + 128].T, axis=0, keepdims=True)

        @pl.when(part == 2)
        def _():
            gather_sums(far, far_sums)

            sent = own_raw.at[pl.ds(0, GROUPS - 1)]
            pltpu.make_async_copy(sent, sent, send_sem).wait()
            lax.fori_loop(0, 8, finish_pass, 0)
            far_copy.start()

        return carry

    lax.fori_loop(0, 4, across, 0)
    gather_sums(near, near_sums)

    lanes_low = lax.broadcasted_iota(jnp.int32, (WIN_DEV, 128), 1) < GROUP_COLS

    def write_out(first, second):
        for p in range(HALF // 128):
            at = pl.ds(p * 128, 128)
            zero = first[0, :, at] + second[0, :, at]
            one = first[1, :, at] + second[1, :, at]
            out_ref[:, pl.ds(2 * p * 128, 128)] = jnp.where(lanes_low, zero, pltpu.roll(one, GROUP_COLS, 1))
            out_ref[:, pl.ds((2 * p + 1) * 128, 128)] = jnp.where(lanes_low, pltpu.roll(zero, GROUP_COLS, 1), one)

    @pl.when(core != half)
    def _():
        near_copy.start()
        for d in range(2):
            pltpu.make_async_copy(arrived.at[d], arrived.at[d], result_recv.at[d]).wait()
        write_out(arrived.at[0], arrived.at[1])
        near_copy.wait_send()

    @pl.when(core == half)
    def _():
        other_core = 1 - core
        pltpu.make_async_copy(arrived.at[other_core], arrived.at[other_core], result_recv.at[other_core]).wait()
        write_out(near_sums, arrived.at[other_core])

    far_copy.wait_send()


def shards(tick_bars, prior_bars):
    return pl.pallas_call(
        kernel,
        out_shape=jax.ShapeDtypeStruct((WIN_DEV, TILE), jnp.float32),
        in_specs=[pl.BlockSpec(memory_space=pl.ANY)] * 2,
        out_specs=pl.BlockSpec(memory_space=pltpu.VMEM),
        scratch_shapes=[
            pltpu.VMEM((SERIES_ROWS, 128), jnp.float32),
            pltpu.VMEM((1, LEAD * GROUP_COLS), jnp.float32),
            pltpu.VMEM((GROUPS, PIECES, 4, 128), jnp.float32),
            pltpu.VMEM((GROUPS, PIECES, 4, 128), jnp.float32),
            pltpu.VMEM((2, 4, 24, 128), jnp.float32),
            pltpu.VMEM((WIN_DEV, 32, 512), jnp.bfloat16),
            pltpu.VMEM((512, 128), jnp.bfloat16),
            pltpu.VMEM((WIN_DEV, 128, TILE), jnp.bfloat16),
            pltpu.VMEM((WIN_DEV, 128, TILE), jnp.bfloat16),
            pltpu.VMEM((TILE, 128), jnp.bfloat16),
            pltpu.VMEM((WIN_DEV, TILE, 128), jnp.float32),
            pltpu.VMEM((WIN_DEV, 8, TILE), jnp.float32),
            pltpu.VMEM((WIN_DEV, 8, TILE), jnp.float32),
            pltpu.VMEM((WIN_DEV, TILE), jnp.float32),
            pltpu.VMEM((2, WIN_DEV, HALF), jnp.float32),
            pltpu.VMEM((2, WIN_DEV, HALF), jnp.float32),
            pltpu.VMEM((2, 2, WIN_DEV, HALF), jnp.float32),
            pltpu.SemaphoreType.DMA((2,)),
            pltpu.SemaphoreType.DMA,
            pltpu.SemaphoreType.DMA((8,)),
            pltpu.SemaphoreType.DMA((8, WIN_DEV)),
            pltpu.SemaphoreType.DMA((8, WIN_DEV)),
            pltpu.SemaphoreType.DMA((2,)),
            pltpu.SemaphoreType.DMA((2,)),
            pltpu.SemaphoreType.REGULAR,
        ],
        compiler_params=pltpu.CompilerParams(collective_id=0, has_side_effects=True, vmem_limit_bytes=56 * 2**20),
        name="connect",
    )(tick_bars.reshape(TICK_ROWS, 128), prior_bars.reshape(1, LEAD * GROUP_COLS))


def solution(mesh):
    in_specs = (P("asset", "tm", None), P("asset", "tm", None))
    out_specs = P("tm", "asset")
    return jax.shard_map(shards, mesh=mesh, in_specs=in_specs, out_specs=out_specs, check_vma=False)
```
